32 devices in a mesh: ctx: 8 (over z, y), dp: 4 (over x, core).
Axes of the slice: x: 2, y: 2, z: 4, core: 2. Of those that a mesh axis runs over, the one named last changes fastest.
Arguments:
- tokens: bfloat16 [8, 512, 4096], P('dp', 'ctx'), may hold values from -6 to 6
- queries: bfloat16 [8, 512, 2048], P('dp', 'ctx'), may hold values from -160 to 160
- d_attended: bfloat16 [8, 512, 2048], P('dp', 'ctx'), may hold values from -6 to 6
- span_order: int32 [16], replicated, may hold values from 0 to 15, each once
- norm_gain: float32 [4096], replicated, may hold values from 0.1 to 1.9
- key_weight: bfloat16 [4096, 512], replicated, may hold values from -0.09375 to 0.09375
- value_weight: bfloat16 [4096, 512], replicated, may hold values from -0.09375 to 0.09375
Outputs:
- attended: bfloat16 [8, 512, 2048], P('dp', 'ctx')
- grad_queries: bfloat16 [8, 512, 2048], P('dp', 'ctx')
- grad_tokens: bfloat16 [8, 512, 4096], P('dp', 'ctx')
- grad_key_weight: float32 [4096, 512], P(('ctx', 'dp'))
- grad_value_weight: float32 [4096, 512], P(('ctx', 'dp'))
- grad_gain: float32 [4096], P(('ctx', 'dp'))
The draws below stay inside these ranges and needn't reach their ends.
All inputs are finite; a program needn't handle non-finite values.
Results may differ from the reference program's by a relative error of at most 0.025.
The reference program's roundings to bfloat16 on the way (of `normed`, `rotated_keys`, `value_rows`, `probability_b`, `dscores`, `key_pre_grad` and `value_pre_grad`) count: a program that leaves them out, or rounds other values in their place, can miss the bound.
Values may be sent and summed in bfloat16 or wider, within the bound.
A program may use at most 192 MiB of HBM per device.

```python
import jax
import jax.numpy as jnp
from jax import lax

D = 4096
HEADS = 16
KV_HEADS = 4
HEAD_DIM = 128
SEQ_DEV = 64
SEQ = 512
SEQS = 8
N_CTX = 8


def draw_queries(key, part):
    full_shape = (SEQS, SEQ, HEADS * HEAD_DIM)
    sample = jnp.clip(jax.random.normal(key, full_shape, jnp.float32), -4.0, 4.0)
    return sample.astype(jnp.bfloat16)


def shard_levels(own_key, extent, shards, smallest, largest):
    factor_of = 1.0
    for axis_at, parts in shards:
        heights = jax.random.uniform(jax.random.fold_in(jax.random.fold_in(own_key, 6), axis_at), (parts,), jnp.float32, smallest / len(shards), largest / len(shards))
        factor_of = factor_of * jnp.repeat(jnp.exp(heights), extent[axis_at] // parts).reshape((-1,) + (1,) * (len(extent) - 1 - axis_at))
    return factor_of


def gaussian(key, shape, scale, limit, shards=(), kind=jnp.bfloat16):
    factor_of = shard_levels(key, shape, shards, -0.22, 0.18) if shards else 1.0
    entries = jax.random.normal(key, shape, jnp.float32) * scale * factor_of
    return jnp.minimum(jnp.maximum(entries, -limit), limit).astype(kind)


def setup_inputs(seed: int = 0) -> dict:
    arg_keys = jax.random.split(jax.random.key(seed), 8)
    return {
        "tokens": gaussian(arg_keys[0], (SEQS, SEQ, D), 1.0, 6.0, ((0, 4), (1, 8))),
        "queries": draw_queries(jax.random.fold_in(arg_keys[7], 71), 0),
        "d_attended": gaussian(arg_keys[2], (SEQS, SEQ, HEADS * HEAD_DIM), 1.0, 6.0, ((0, 4), (1, 8))),
        "span_order": jax.random.permutation(arg_keys[3], 2 * N_CTX).astype(jnp.int32),
        "norm_gain": jnp.clip(1.0 + 0.18 * jax.random.normal(arg_keys[4], (D,), jnp.float32), 0.1, 1.9),
        "key_weight": gaussian(arg_keys[5], (D, KV_HEADS * HEAD_DIM), D ** -0.5, 0.09375),
        "value_weight": gaussian(arg_keys[6], (D, KV_HEADS * HEAD_DIM), D ** -0.5, 0.09375),
    }


ROPE_BASE = 500000.0
EPSILON = 1e-05

def positions(span_order, span_len):
    offsets = jnp.arange(span_len, dtype=jnp.int32)
    return (span_order[:, None] * span_len + offsets[None, :]).reshape(-1).astype(jnp.int32)

def rotation(token_pos, head_size):
    half_dim = head_size // 2
    frequency = ROPE_BASE ** (-2.0 * jnp.arange(half_dim, dtype=jnp.float32) / head_size)
    angles = token_pos.astype(jnp.float32)[:, None] * frequency[None, :]
    angles = jnp.concatenate([angles, angles], axis=1)
    return (jnp.cos(angles), jnp.sin(angles))

def rotate_half(values):
    half_dim = values.shape[-1] // 2
    return jnp.concatenate([-values[..., half_dim:], values[..., :half_dim]], axis=-1)

def rotate_back(values):
    half_dim = values.shape[-1] // 2
    return jnp.concatenate([values[..., half_dim:], -values[..., :half_dim]], axis=-1)

def normalize(tokens, norm_gain):
    widened = tokens.astype(jnp.float32)
    rms_scale = lax.rsqrt(lax.optimization_barrier(jnp.mean(widened * widened, axis=-1, keepdims=True)) + EPSILON)
    return ((widened * rms_scale * norm_gain).astype(jnp.bfloat16), rms_scale)

def project_keys(normed, key_weight, value_weight, cosine, sine_table, kv_heads, head_size):
    row_count = normed.shape[0]
    key_pre = jnp.dot(normed, key_weight, preferred_element_type=jnp.float32).reshape(row_count, kv_heads, head_size)
    rotated = key_pre * cosine[:, None, :] + rotate_half(key_pre) * sine_table[:, None, :]
    value_rows = jnp.dot(normed, value_weight, preferred_element_type=jnp.float32)
    return (rotated.reshape(row_count, kv_heads * head_size).astype(jnp.bfloat16), value_rows.astype(jnp.bfloat16))

def attend_group(query_group, grad_group, key_group, value_group, causal_mask, score_scale):
    query_wide = query_group.astype(jnp.float32)
    grad_wide = grad_group.astype(jnp.float32)
    key_wide = key_group.astype(jnp.float32)
    value_wide = value_group.astype(jnp.float32)
    scores = jnp.einsum('tgd,sd->gts', query_wide, key_wide) * score_scale
    scores = jnp.where(causal_mask[None], scores, -1e+30)
    row_max = lax.optimization_barrier(jnp.max(scores, axis=-1, keepdims=True))
    exponent = jnp.exp(scores - row_max)
    probability = exponent / lax.optimization_barrier(jnp.sum(exponent, axis=-1, keepdims=True))
    probability_b = probability.astype(jnp.bfloat16)
    prob_wide = probability_b.astype(jnp.float32)
    attended = jnp.einsum('gts,sd->tgd', prob_wide, value_wide).astype(jnp.bfloat16)
    dprob = jnp.einsum('tgd,sd->gts', grad_wide, value_wide)
    delta = lax.optimization_barrier(jnp.sum(grad_wide * attended.astype(jnp.float32), axis=-1))
    dscores = (probability * (dprob - jnp.transpose(delta)[:, :, None])).astype(jnp.bfloat16)
    dscore_wide = dscores.astype(jnp.float32)
    dquery = (jnp.einsum('gts,sd->tgd', dscore_wide, key_wide) * score_scale).astype(jnp.bfloat16)
    key_term = jnp.einsum('gts,tgd->sd', dscore_wide, query_wide) * score_scale
    value_term = jnp.einsum('gts,tgd->sd', prob_wide, grad_wide)
    return (attended, dquery, key_term, value_term)

def attend_device(queries, grads, all_keys, all_values, query_pos, key_pos, kv_heads, head_size):
    row_count = queries.shape[0]
    group_size = queries.shape[1] // (kv_heads * head_size)
    group_width = group_size * head_size
    causal_mask = key_pos[None, :] <= query_pos[:, None]
    score_scale = head_size ** (-0.5)
    outputs = []
    for head_group in range(kv_heads):
        query_group = queries[:, head_group * group_width:(head_group + 1) * group_width].reshape(row_count, group_size, head_size)
        grad_group = grads[:, head_group * group_width:(head_group + 1) * group_width].reshape(row_count, group_size, head_size)
        key_group = all_keys[:, head_group * head_size:(head_group + 1) * head_size]
        value_group = all_values[:, head_group * head_size:(head_group + 1) * head_size]
        outputs.append(attend_group(query_group, grad_group, key_group, value_group, causal_mask, score_scale))
    attended = jnp.concatenate([item[0].reshape(row_count, group_width) for item in outputs], axis=1)
    dquery = jnp.concatenate([item[1].reshape(row_count, group_width) for item in outputs], axis=1)
    key_terms = jnp.concatenate([item[2] for item in outputs], axis=1)
    value_terms = jnp.concatenate([item[3] for item in outputs], axis=1)
    return (attended, dquery, key_terms, value_terms)

def finish_backward(tokens, normed, rms_scale, key_grad, value_grad, cosine, sine_table, norm_gain, key_weight, value_weight, kv_heads, head_size):
    row_count = tokens.shape[0]
    shaped = key_grad.reshape(row_count, kv_heads, head_size)
    key_pre_grad = (shaped * cosine[:, None, :] + rotate_back(shaped * sine_table[:, None, :])).reshape(row_count, kv_heads * head_size).astype(jnp.bfloat16)
    value_pre_grad = value_grad.astype(jnp.bfloat16)
    weight_key = jnp.dot(normed.T, key_pre_grad, preferred_element_type=jnp.float32)
    weight_value = jnp.dot(normed.T, value_pre_grad, preferred_element_type=jnp.float32)
    normed_grad = jnp.dot(key_pre_grad, key_weight.T, preferred_element_type=jnp.float32) + jnp.dot(value_pre_grad, value_weight.T, preferred_element_type=jnp.float32)
    widened = tokens.astype(jnp.float32)
    gain_part = lax.optimization_barrier(jnp.sum(normed_grad * widened * rms_scale, axis=0))
    inner_mean = lax.optimization_barrier(jnp.mean(normed_grad * norm_gain * widened, axis=-1, keepdims=True))
    grad_rows = (rms_scale * norm_gain * normed_grad - widened * rms_scale ** 3 * inner_mean).astype(jnp.bfloat16)
    return (grad_rows, weight_key, weight_value, gain_part)

def reference(tokens, queries, d_attended, span_order, norm_gain, key_weight, value_weight):
    token_pos = positions(span_order, SEQ_DEV // 2)
    cosine, sine_table = rotation(token_pos, HEAD_DIM)
    kv_width = KV_HEADS * HEAD_DIM
    total_key = jnp.zeros((D, kv_width), jnp.float32)
    total_value = jnp.zeros((D, kv_width), jnp.float32)
    total_gain = jnp.zeros((D,), jnp.float32)
    attended_list, dquery_list, dtoken_list = ([], [], [])
    for sequence in range(SEQS):
        normed, rms_scale = normalize(tokens[sequence], norm_gain)
        rotated_keys, value_rows = project_keys(normed, key_weight, value_weight, cosine, sine_table, KV_HEADS, HEAD_DIM)
        seq_queries = queries[sequence]
        seq_grads = d_attended[sequence]

        def shard_step(totals, shard_index):
            first_row = shard_index * SEQ_DEV
            block_queries = lax.dynamic_slice_in_dim(seq_queries, first_row, SEQ_DEV, 0)
            block_grads = lax.dynamic_slice_in_dim(seq_grads, first_row, SEQ_DEV, 0)
            query_pos = lax.dynamic_slice_in_dim(token_pos, first_row, SEQ_DEV, 0)
            attended, dquery, key_terms, value_terms = attend_device(block_queries, block_grads, rotated_keys, value_rows, query_pos, token_pos, KV_HEADS, HEAD_DIM)
            key_round = lax.optimization_barrier(key_terms.astype(jnp.bfloat16)).astype(jnp.float32)
            value_round = lax.optimization_barrier(value_terms.astype(jnp.bfloat16)).astype(jnp.float32)
            return ((totals[0] + key_round, totals[1] + value_round), (attended, dquery))
        zeros_init = jnp.zeros((SEQ, kv_width), jnp.float32)
        sums, stacked = lax.scan(shard_step, (zeros_init, zeros_init), jnp.arange(N_CTX, dtype=jnp.int32))
        attended_list.append(stacked[0].reshape(SEQ, HEADS * HEAD_DIM))
        dquery_list.append(stacked[1].reshape(SEQ, HEADS * HEAD_DIM))
        grad_rows, weight_key, weight_value, gain_part = finish_backward(tokens[sequence], normed, rms_scale, sums[0], sums[1], cosine, sine_table, norm_gain, key_weight, value_weight, KV_HEADS, HEAD_DIM)
        dtoken_list.append(grad_rows)
        total_key = total_key + weight_key
        total_value = total_value + weight_value
        total_gain = total_gain + gain_part
    return (jnp.stack(attended_list), jnp.stack(dquery_list), jnp.stack(dtoken_list), total_key, total_value, total_gain)
```

```python
import functools

import jax
import jax.numpy as jnp
import numpy as np
from jax import lax
from jax.experimental import pallas as pl
from jax.experimental.pallas import tpu as pltpu
from jax.sharding import PartitionSpec as P

HEAD_DIM = 128
ROPE_BASE = 500000.0
EPSILON = 1e-05
MESH = pl.DeviceIdType.MESH
VMEM = pl.BlockSpec(memory_space=pltpu.VMEM)
SMEM = pl.BlockSpec(memory_space=pltpu.SMEM)
ANY = pl.BlockSpec(memory_space=pl.ANY)
F32 = jnp.float32
BF16 = jnp.bfloat16
LIMIT = 60 * 1024 * 1024

PARTS = 2
PIECES = 4

MESSAGE = 1.4
LATENCY = 2.2


def ring_place(index, n):
    return jnp.where(index % 2 == 0, index // 2, n - 1 - index // 2)


def ring_index(place, n):
    place = (place + 2 * n) % n
    return jnp.where(place < n // 2, 2 * place, 2 * (n - 1 - place) + 1)


def remote(src, dst, send, recv, axis, target):
    return pltpu.make_async_remote_copy(
        src_ref=src,
        dst_ref=dst,
        send_sem=send,
        recv_sem=recv,
        device_id={axis: target},
        device_id_type=MESH,
    )


def rotation_tables(spans, span_len):
    half = HEAD_DIM // 2
    frequency = ROPE_BASE ** (-2.0 * np.arange(half, dtype=np.float64) / HEAD_DIM)
    frequency = np.concatenate([frequency, frequency])

    def table(at):
        angle = at.astype(np.float64)[:, None] * frequency[None, :]
        return np.stack([np.cos(angle), np.sin(angle)]).astype(np.float32)

    return table(np.arange(spans) * span_len), table(np.arange(span_len))


class Task:
    def __init__(self, name, rank, cost, emit, needs=(), waits=(), sends=()):
        self.name, self.rank, self.cost, self.emit = name, rank, cost, emit
        self.needs, self.waits, self.sends = needs, waits, sends


def arrange(tasks):
    now, free, arrival, done, order = 0.0, {}, {}, set(), []
    left = list(tasks)
    while left:
        best = None
        for task in left:
            if all(name in done for name in task.needs) and all(key in arrival for key in task.waits):
                at = max([arrival[key] for key in task.waits], default=0.0)
                key = (max(at, now), task.rank)
                if best is None or key < best[0]:
                    best = (key, task)
        (at, _), task = best
        left.remove(task)
        now = at + task.cost
        done.add(task.name)
        order.append((at, task))
        for key, link, cost in task.sends:
            free[link] = max(free.get(link, 0.0), now) + cost
            arrival[key] = free[link] + LATENCY
    return order


def blocks_of(n, m, own, permuted):
    if permuted:
        return [(j * n * own, n * own, j, 0) for j in range(m)]
    return [(b * own, own, b % m, (b // m) * own) for b in range(n * m)]


def layer_kernel(
    n,
    m,
    permuted,
    span_ref,
    start_ref,
    offset_ref,
    gain_ref,
    gain_rows,
    x_hbm,
    wk_hbm,
    wv_hbm,
    q_hbm,
    g_hbm,
    att,
    dq,
    gx,
    gkw,
    gvw,
    gain_out,
    x_ref,
    wk,
    wv,
    q_ref,
    g_ref,
    normed,
    xg,
    xt,
    kv,
    terms,
    inbox,
    gall,
    own_k,
    own_v,
    part2,
    mine,
    inbox2,
    rms_ref,
    ng,
    cos_ref,
    sin_ref,
    bias,
    xsem,
    wsem,
    qsem,
    a_send,
    a_recv,
    r_send,
    r_recv,
    w_send,
    w_recv,
    x_send,
    x_recv,
    g_send,
    g_recv,
):
    me = lax.axis_index("ctx")
    dp = lax.axis_index("dp")
    place = ring_place(me, n)
    sign = (1, -1)
    targets = [ring_index(place + 1, n), ring_index(place - 1, n)]
    seqs, rows, _ = q_ref.shape
    kv_width = wk.shape[1]
    model_width = x_ref.shape[2]
    count = seqs * rows
    own = gkw.shape[0]
    head = HEAD_DIM
    span_len = rows // 2
    width = kv_width // PARTS
    heads = width // head
    group = q_ref.shape[2] // kv_width
    scale = head ** (-0.5)
    units = PARTS * seqs
    half_own = own // 2
    nt = (((1,), (1,)), ((), ()))
    nn = (((1,), (0,)), ((), ()))
    tn = (((0,), (0,)), ((), ()))
    dot = functools.partial(lax.dot_general, preferred_element_type=F32)
    blocks = blocks_of(n, m, own, permuted)
    per_piece = len(blocks) // PIECES
    piece_width = model_width // PIECES

    x_loads = [pltpu.make_async_copy(x_hbm.at[c], x_ref.at[c], xsem.at[c]) for c in range(seqs)]
    for load in x_loads:
        load.start()
    w_loads = []
    for q in range(PIECES):
        at = pl.ds(q * piece_width, piece_width)
        pair = [
            pltpu.make_async_copy(src.at[at], dst.at[at], wsem.at[t, q])
            for t, (src, dst) in enumerate(((wk_hbm, wk), (wv_hbm, wv)))
        ]
        for load in pair:
            load.start()
        w_loads.append(pair)
    q_loads = [
        pltpu.make_async_copy(src, dst, qsem.at[t])
        for t, (src, dst) in enumerate(((q_hbm, q_ref), (g_hbm, g_ref)))
    ]
    for load in q_loads:
        load.start()
    barrier = pltpu.get_barrier_semaphore()
    for axis, target in [("ctx", targets[0]), ("ctx", targets[1])] + [("dp", (dp + o) % m) for o in range(1, m)]:
        pl.semaphore_signal(barrier, inc=1, device_id={axis: target}, device_id_type=MESH)

    offset_cos, offset_sin = offset_ref[0], offset_ref[1]
    lane = lax.broadcasted_iota(jnp.int32, (span_len, head), 1)
    signs = jnp.where(lane < head // 2, -1.0, 1.0).astype(F32)
    for half in range(2):
        span = span_ref[2 * me + half]
        start_cos = start_ref[0, pl.ds(span, 1), :]
        start_sin = start_ref[1, pl.ds(span, 1), :]
        at = slice(half * span_len, (half + 1) * span_len)
        cos_ref[at] = start_cos * offset_cos - start_sin * offset_sin
        sin_ref[at] = (start_sin * offset_cos + start_cos * offset_sin) * signs

    for c in range(seqs):
        x_loads[c].wait()
        total = jnp.zeros((rows, 1), F32)
        for q in range(PIECES):
            wide = x_ref[c, :, q * piece_width : (q + 1) * piece_width].astype(F32)
            total = total + jnp.sum(wide * wide, axis=1, keepdims=True)
        rms = lax.rsqrt(total / model_width + EPSILON)
        rms_ref[c] = rms
        for start, size, j, offset in blocks:
            at = slice(start, start + size)
            value = (x_ref[c, :, at].astype(F32) * rms * gain_ref[:, at]).astype(BF16)
            normed[j, c, :, offset : offset + size] = value

    key = jnp.zeros((count, kv_width), F32)
    value = jnp.zeros((count, kv_width), F32)
    for q in range(PIECES):
        lhs = jnp.concatenate(
            [
                normed[j, :, :, offset : offset + size].reshape(count, size)
                for _, size, j, offset in blocks[q * per_piece : (q + 1) * per_piece]
            ],
            axis=1,
        )
        for load in w_loads[q]:
            load.wait()
        at = slice(q * piece_width, (q + 1) * piece_width)
        key = key + dot(lhs, wk[at], nn)
        value = value + dot(lhs, wv[at], nn)
    for u in range(units):
        part, c = divmod(u, seqs)
        for k in range(heads):
            col = part * width + k * head
            turn = key[c * rows : (c + 1) * rows, col : col + head]
            turned = pltpu.roll(turn, head // 2, 1)
            kv[u, me, :, k * head : (k + 1) * head] = (turn * cos_ref[...] + turned * sin_ref[...]).astype(BF16)
        kv[u, me, :, width : 2 * width] = value[
            c * rows : (c + 1) * rows, part * width : (part + 1) * width
        ].astype(BF16)
    pl.semaphore_wait(barrier, 2 + m - 1)

    def hops(d, parity):
        return n // 2 if d == parity else n // 2 - 1

    def a_copy(u, d, s):
        slot = kv.at[u, ring_index(place - sign[d] * s, n)]
        return remote(slot, slot, a_send.at[u, d, s], a_recv.at[u, d, s], "ctx", targets[d])

    def a_arrive(u, d, s):
        slot = kv.at[u, ring_index(place - sign[d] * (s + 1), n)]
        remote(slot, slot, a_send.at[u, d, s], a_recv.at[u, d, s], "ctx", targets[d]).wait_recv()

    def r_copy(u, d, s):
        if s == 0:
            src = terms.at[u, ring_index(place + sign[d] * hops(d, u % 2), n)]
        else:
            src = inbox.at[u, d, s - 1]
        return remote(src, inbox.at[u, d, s], r_send.at[u, d, s], r_recv.at[u, d, s], "ctx", targets[d])

    def r_arrive(u, d, s):
        slot = inbox.at[u, d, s]
        remote(slot, slot, r_send.at[u, d, s], r_recv.at[u, d, s], "ctx", targets[d]).wait_recv()

    def w_copy(part, half, d, s):
        lane = 2 * part + half
        if s == 0:
            owner = ring_index(place + sign[d] * hops(d, half), n)
            src = part2.at[part, owner, pl.ds(half * half_own, half_own)]
        else:
            src = inbox2.at[lane, d, s - 1]
        return remote(src, inbox2.at[lane, d, s], w_send.at[lane, d, s], w_recv.at[lane, d, s], "ctx", targets[d])

    def w_arrive(part, half, d, s):
        lane = 2 * part + half
        slot = inbox2.at[lane, d, s]
        remote(slot, slot, w_send.at[lane, d, s], w_recv.at[lane, d, s], "ctx", targets[d]).wait_recv()

    def x_copy(o):
        target = (dp + o) % m
        return remote(normed.at[target], xg.at[:, dp], x_send.at[o - 1], x_recv.at[o - 1], "dp", target)

    def x_arrive(o):
        slot = xg.at[:, (dp + m - o) % m]
        remote(slot, slot, x_send.at[o - 1], x_recv.at[o - 1], "dp", (dp + o) % m).wait_recv()

    def g_copy(u, o):
        slot = gall.at[u, dp]
        return remote(slot, slot, g_send.at[u, o - 1], g_recv.at[u, o - 1], "dp", (dp + o) % m)

    def g_arrive(u, o):
        slot = gall.at[u, (dp + m - o) % m]
        remote(slot, slot, g_send.at[u, o - 1], g_recv.at[u, o - 1], "dp", (dp + o) % m).wait_recv()

    tasks = []

    def task(name, rank, cost, emit, **rest):
        tasks.append(Task(name, rank, cost, emit, **rest))

    def a_step(u, d, s):
        if s > 0:
            a_arrive(u, d, s - 1)
        a_copy(u, d, s).start()

    for s in range(n // 2):
        for u in range(units):
            for d in range(2):
                if s < hops(d, u % 2):
                    task(
                        ("A", u, d, s),
                        0 + s + u / units,
                        0.02,
                        functools.partial(a_step, u, d, s),
                        needs=[("A", v, d, 0) for v in range(u)] if s == 0 else [],
                        waits=[("A", u, d, s - 1)] if s > 0 else [],
                        sends=[(("A", u, d, s), d, MESSAGE)],
                    )

    def x_step():
        for o in range(1, m):
            x_copy(o).start()
        xg[:, dp] = normed[dp]

    task("X", 0.9, 0.15, x_step, sends=[(("X", o), "x", 2 * MESSAGE) for o in range(1, m)])

    def mask_step():
        for load in q_loads:
            load.wait()
        spans = 2 * n
        lane = lax.broadcasted_iota(jnp.int32, (1, n * rows), 1)
        key_pos = jnp.zeros((1, n * rows), jnp.int32)
        for k in range(spans):
            inside = (lane >= k * span_len) & (lane < (k + 1) * span_len)
            key_pos = jnp.where(inside, lane + (span_ref[k] - k) * span_len, key_pos)
        row = lax.broadcasted_iota(jnp.int32, (rows, 1), 0)
        first, second = span_ref[2 * me], span_ref[2 * me + 1]
        query_pos = row + jnp.where(row < span_len, first * span_len, (second - 1) * span_len)
        bias[...] = jnp.where(key_pos <= query_pos, 0.0, -1e30).astype(F32)

    task("mask", 40, 0.2, mask_step)

    def transpose_step(c):
        wide = xg[c].reshape(m * rows, n * own)
        xt[c] = jnp.transpose(wide).reshape(n, own, m * rows)

    def x_wait():
        for o in range(1, m):
            x_arrive(o)

    task("xwait", 45, 0.02, x_wait, waits=[("X", o) for o in range(1, m)])
    for c in range(seqs):
        task(("xt", c), 50 + c, 0.7, functools.partial(transpose_step, c), needs=["xwait"])

    def attend_step(u, k):
        part, c = divmod(u, seqs)
        if k == 0:
            for d in range(2):
                a_arrive(u, d, hops(d, u % 2) - 1)
        first = ((part * heads + k) * group) * head
        columns = [slice(first + i * head, first + (i + 1) * head) for i in range(group)]
        query = jnp.concatenate([q_ref[c, :, column] for column in columns], axis=0)
        grad = jnp.concatenate([g_ref[c, :, column] for column in columns], axis=0)
        key_at = slice(k * head, (k + 1) * head)
        value_at = slice(width + k * head, width + (k + 1) * head)
        key = kv[u, :, :, key_at].reshape(n * rows, head)
        value = kv[u, :, :, value_at].reshape(n * rows, head)
        masked = jnp.concatenate([bias[...]] * group, axis=0)
        scores = dot(query, key, nt) * scale + masked
        exponent = jnp.exp(scores - jnp.max(scores, axis=1, keepdims=True))
        probability = exponent * (1.0 / jnp.sum(exponent, axis=1, keepdims=True))
        rounded = probability.astype(BF16)
        attended = dot(rounded, value, nn).astype(BF16)
        delta = jnp.sum(grad.astype(F32) * attended.astype(F32), axis=1, keepdims=True)
        dscores = (probability * (dot(grad, value, nt) - delta)).astype(BF16)
        dquery = (dot(dscores, key, nn) * scale).astype(BF16)
        for i in range(group):
            att[c, :, columns[i]] = attended[i * rows : (i + 1) * rows]
            dq[c, :, columns[i]] = dquery[i * rows : (i + 1) * rows]
        terms[u, :, :, key_at] = (dot(dscores, query, tn) * scale).astype(BF16).reshape(n, rows, head)
        terms[u, :, :, value_at] = dot(rounded, grad, tn).astype(BF16).reshape(n, rows, head)

    for u in range(units):
        for k in range(heads):
            task(
                ("attend", u, k),
                20 + u + k / heads,
                0.95,
                functools.partial(attend_step, u, k),
                needs=["mask"] if k == 0 else [("attend", u, k - 1)],
                waits=[("A", u, d, hops(d, u % 2) - 1) for d in range(2)] if k == 0 else [],
            )

    def r_step(u, d, s):
        if s > 0:
            r_arrive(u, d, s - 1)
            owner = ring_index(place + sign[d] * (hops(d, u % 2) - s), n)
            inbox[u, d, s - 1] = (inbox[u, d, s - 1].astype(F32) + terms[u, owner].astype(F32)).astype(BF16)
        r_copy(u, d, s).start()

    def r_total(u):
        part, c = divmod(u, seqs)
        result = terms[u, me].astype(F32)
        for d in (1 - u % 2, u % 2):
            last = hops(d, u % 2) - 1
            r_arrive(u, d, last)
            result = result + inbox[u, d, last].astype(F32)
        at = slice(c * rows, (c + 1) * rows)
        for k in range(heads):
            back = result[:, k * head : (k + 1) * head]
            turned = pltpu.roll(back, head // 2, 1)
            back = (back * cos_ref[...] - turned * sin_ref[...]).astype(BF16)
            gall[u, dp, :, k * head : (k + 1) * head] = back
            own_k[at, part * width + k * head : part * width + (k + 1) * head] = back
        back = result[:, width:].astype(BF16)
        gall[u, dp, :, width:] = back
        own_v[at, part * width : (part + 1) * width] = back
        for o in range(1, m):
            g_copy(u, o).start()

    for u in range(units):
        for s in range(n // 2):
            for d in range(2):
                if s < hops(d, u % 2):
                    task(
                        ("R", u, d, s),
                        5 + s + u / units,
                        0.1 if s else 0.02,
                        functools.partial(r_step, u, d, s),
                        needs=[] if s else [("attend", u, heads - 1)],
                        waits=[("R", u, d, s - 1)] if s else [],
                        sends=[(("R", u, d, s), d, MESSAGE)],
                    )
        task(
            ("total", u),
            4 + u / units,
            0.25,
            functools.partial(r_total, u),
            waits=[("R", u, d, hops(d, u % 2) - 1) for d in range(2)],
            sends=[(("G", u, o), "x", MESSAGE) for o in range(1, m)],
        )

    def g_wait(u):
        for o in range(1, m):
            g_arrive(u, o)

    for u in range(units):
        task(("gwait", u), 10, 0.02, functools.partial(g_wait, u), waits=[("G", u, o) for o in range(1, m)])

    def product_step(part, offset):
        owner = ring_index(place + offset, n)
        total = jnp.zeros((own, 2 * width), F32)
        for c in range(seqs):
            total = total + dot(xt[c, owner], gall[part * seqs + c].reshape(m * rows, 2 * width), nn)
        if offset == 0:
            mine[part] = total
        else:
            part2[part, owner] = total.astype(BF16)

    def centred(offset):
        return offset + n if offset <= -(n // 2) else offset

    for part in range(PARTS):
        for i, offset in enumerate(sorted(range(-(n // 2) + 1, n // 2 + 1), key=lambda v: (-abs(v), v))):
            task(
                ("M", part, offset),
                11 + part + i / 100,
                0.15,
                functools.partial(product_step, part, offset),
                needs=[("gwait", part * seqs + c) for c in range(seqs)] + [("xt", c) for c in range(seqs)],
            )

    def w_step(part, half, d, s):
        if s > 0:
            w_arrive(part, half, d, s - 1)
            lane = 2 * part + half
            owner = ring_index(place + sign[d] * (hops(d, half) - s), n)
            mid = part2[part, owner, half * half_own : (half + 1) * half_own]
            inbox2[lane, d, s - 1] = (inbox2[lane, d, s - 1].astype(F32) + mid.astype(F32)).astype(BF16)
        w_copy(part, half, d, s).start()

    def w_total(part, half):
        lane = 2 * part + half
        at = slice(half * half_own, (half + 1) * half_own)
        result = mine[part, at]
        for d in (1 - half, half):
            last = hops(d, half) - 1
            w_arrive(part, half, d, last)
            result = result + inbox2[lane, d, last].astype(F32)
        gkw[at, part * width : (part + 1) * width] = result[:, :width]
        gvw[at, part * width : (part + 1) * width] = result[:, width:]

    for part in range(PARTS):
        for half in range(2):
            for s in range(n // 2):
                for d in range(2):
                    if s < hops(d, half):
                        task(
                            ("W", part, half, d, s),
                            2 + part + s / 10,
                            0.1 if s else 0.02,
                            functools.partial(w_step, part, half, d, s),
                            needs=[("M", part, centred(sign[d] * (hops(d, half) - s)))],
                            waits=[("W", part, half, d, s - 1)] if s else [],
                            sends=[(("W", part, half, d, s), d, MESSAGE)],
                        )
            task(
                ("wtotal", part, half),
                3,
                0.15,
                functools.partial(w_total, part, half),
                needs=[("M", part, 0)],
                waits=[("W", part, half, d, hops(d, half) - 1) for d in range(2)],
            )

    state = {}

    def project_step(q):
        at = slice(q * piece_width, (q + 1) * piece_width)
        piece = dot(own_k[...], wk[at], nt) + dot(own_v[...], wv[at], nt)
        ng[:, at] = piece
        wide = x_ref[:, :, at].reshape(count, piece_width).astype(F32)
        inner = jnp.sum(piece * gain_ref[:, at] * wide, axis=1, keepdims=True)
        state["inner"] = state["inner"] + inner if q else inner

    def finish_step(q):
        at = slice(q * piece_width, (q + 1) * piece_width)
        rms = rms_ref[...].reshape(count, 1)
        slope = rms * rms * rms * (state["inner"] / model_width)
        wide = x_ref[:, :, at].reshape(count, piece_width).astype(F32)
        gx[:, at] = (rms * gain_ref[:, at] * ng[:, at] - wide * slope).astype(BF16)

    for q in range(PIECES):
        task(
            ("project", q),
            60 + q,
            0.9,
            functools.partial(project_step, q),
            needs=[("total", u) for u in range(units)] + ([("project", q - 1)] if q else []),
        )
        task(("finish", q), 70 + q, 0.25, functools.partial(finish_step, q), needs=[("project", PIECES - 1)])

    order = arrange(tasks)
    for _, item in order:
        item.emit()

    block = dp * n + me if permuted else me * m + dp
    at = pl.ds(pl.multiple_of(block * own, own), own)
    both = wk[at].astype(F32) * gkw[...] + wv[at].astype(F32) * gvw[...]
    folded = both[:, :128]
    for q in range(1, kv_width // 128):
        folded = folded + both[:, q * 128 : (q + 1) * 128]
    gain_out[...] = jnp.sum(jnp.transpose(folded), axis=0, keepdims=True) / gain_rows[pl.ds(block, 1), :]

    for s in range(n // 2):
        for d in range(2):
            for u in range(units):
                if s < hops(d, u % 2):
                    a_copy(u, d, s).wait_send()
                    r_copy(u, d, s).wait_send()
            for part in range(PARTS):
                for half in range(2):
                    if s < hops(d, half):
                        w_copy(part, half, d, s).wait_send()
    for o in range(1, m):
        x_copy(o).wait_send()
        for u in range(units):
            g_copy(u, o).wait_send()


def layer(n, m, permuted, span_order, norm_gain, tokens, key_weight, value_weight, queries, grads):
    seqs, rows, model_width = tokens.shape
    kv_width = key_weight.shape[1]
    own = model_width // (n * m)
    width = kv_width // PARTS
    units = PARTS * seqs
    count = seqs * rows
    starts, offsets = rotation_tables(2 * n, rows // 2)
    dma = pltpu.SemaphoreType.DMA
    ring = dma((units, 2, n // 2))
    lanes = dma((2 * PARTS, 2, n // 2))
    return pl.pallas_call(
        functools.partial(layer_kernel, n, m, permuted),
        out_shape=(
            jax.ShapeDtypeStruct(queries.shape, BF16),
            jax.ShapeDtypeStruct(queries.shape, BF16),
            jax.ShapeDtypeStruct((count, model_width), BF16),
            jax.ShapeDtypeStruct((own, kv_width), F32),
            jax.ShapeDtypeStruct((own, kv_width), F32),
            jax.ShapeDtypeStruct((1, own), F32),
        ),
        in_specs=[SMEM] + [VMEM] * 4 + [ANY] * 5,
        out_specs=[VMEM] * 6,
        scratch_shapes=[
            pltpu.VMEM(tokens.shape, BF16),
            pltpu.VMEM(key_weight.shape, BF16),
            pltpu.VMEM(value_weight.shape, BF16),
            pltpu.VMEM(queries.shape, BF16),
            pltpu.VMEM(queries.shape, BF16),
            pltpu.VMEM((m, seqs, rows, n * own), BF16),
            pltpu.VMEM((seqs, m, rows, n * own), BF16),
            pltpu.VMEM((seqs, n, own, m * rows), BF16),
            pltpu.VMEM((units, n, rows, 2 * width), BF16),
            pltpu.VMEM((units, n, rows, 2 * width), BF16),
            pltpu.VMEM((units, 2, n // 2, rows, 2 * width), BF16),
            pltpu.VMEM((units, m, rows, 2 * width), BF16),
            pltpu.VMEM((count, kv_width), BF16),
            pltpu.VMEM((count, kv_width), BF16),
            pltpu.VMEM((PARTS, n, own, 2 * width), BF16),
            pltpu.VMEM((PARTS, own, 2 * width), F32),
            pltpu.VMEM((2 * PARTS, 2, n // 2, own // 2, 2 * width), BF16),
            pltpu.VMEM((seqs, rows, 1), F32),
            pltpu.VMEM((count, model_width), F32),
            pltpu.VMEM((rows, HEAD_DIM), F32),
            pltpu.VMEM((rows, HEAD_DIM), F32),
            pltpu.VMEM((rows, n * rows), F32),
            dma((seqs,)),
            dma((2, PIECES)),
            dma((2,)),
            ring,
            ring,
            ring,
            ring,
            lanes,
            lanes,
            dma((m - 1,)),
            dma((m - 1,)),
            dma((units, m - 1)),
            dma((units, m - 1)),
        ],
        compiler_params=pltpu.CompilerParams(
            collective_id=0, has_side_effects=True, vmem_limit_bytes=LIMIT
        ),
        name="layer",
    )(
        span_order,
        jnp.asarray(starts),
        jnp.asarray(offsets),
        norm_gain[None, :],
        norm_gain.reshape(n * m, own),
        tokens,
        key_weight,
        value_weight,
        queries,
        grads,
    )


def deliver_kernel(*refs):
    count = (len(refs) - 1) // 2
    sems = refs[-1]
    copies = [pltpu.make_async_copy(refs[i], refs[count + i], sems.at[i]) for i in range(count)]
    for copy in copies:
        copy.start()
    for copy in copies:
        copy.wait()


def deliver(*arrays):
    return pl.pallas_call(
        deliver_kernel,
        out_shape=tuple(jax.ShapeDtypeStruct(a.shape, a.dtype) for a in arrays),
        in_specs=[VMEM] * len(arrays),
        out_specs=[ANY] * len(arrays),
        scratch_shapes=[pltpu.SemaphoreType.DMA((len(arrays),))],
        compiler_params=pltpu.CompilerParams(vmem_limit_bytes=LIMIT),
        name="deliver",
    )(*arrays)


def body(n, m, tokens, queries, d_attended, span_order, norm_gain, key_weight, value_weight):
    seqs, rows, model_width = tokens.shape
    own = model_width // (n * m)
    permuted = own % 128 != 0

    def shuffle(array, axis):
        shape = array.shape
        split = array.reshape(shape[:axis] + (n, m, own) + shape[axis + 1 :])
        return jnp.swapaxes(split, axis, axis + 1).reshape(shape)

    if permuted:
        tokens, norm_gain = shuffle(tokens, 2), shuffle(norm_gain, 0)
        key_weight, value_weight = shuffle(key_weight, 0), shuffle(value_weight, 0)
    attended, dquery, grad_rows, key_grad, value_grad, gain = deliver(
        *layer(n, m, permuted, span_order, norm_gain, tokens, key_weight, value_weight, queries, d_attended)
    )
    grad_rows = grad_rows.reshape(seqs, rows, model_width)
    if permuted:
        split = grad_rows.reshape(seqs, rows, m, n, own)
        grad_rows = jnp.swapaxes(split, 2, 3).reshape(seqs, rows, model_width)
    return attended, dquery, grad_rows, key_grad, value_grad, gain.reshape(own)


def solution(mesh):
    split = P("dp", "ctx", None)
    return jax.shard_map(
        functools.partial(body, mesh.shape["ctx"], mesh.shape["dp"]),
        mesh=mesh,
        in_specs=(split, split, split, P(), P(), P(), P()),
        out_specs=(
            split,
            split,
            split,
            P(("ctx", "dp"), None),
            P(("ctx", "dp"), None),
            P(("ctx", "dp")),
        ),
        check_vma=False,
    )
```

```python
import functools

import jax
import jax.numpy as jnp
import numpy as np
from jax import lax
from jax.experimental import pallas as pl
from jax.experimental.pallas import tpu as pltpu
from jax.sharding import PartitionSpec as P

HEAD_DIM = 128
ROPE_BASE = 500000.0
EPSILON = 1e-05
MESH = pl.DeviceIdType.MESH
VMEM = pl.BlockSpec(memory_space=pltpu.VMEM)
HBM = pl.BlockSpec(memory_space=pltpu.HBM)
ANY = pl.BlockSpec(memory_space=pl.ANY)
F32 = jnp.float32
BF16 = jnp.bfloat16
MIB = 1024 * 1024

PARTS = 4
PIECES = 4


def ring_place(index, n):
    return jnp.where(index % 2 == 0, index // 2, n - 1 - index // 2)


def ring_index(place, n):
    place = (place + 2 * n) % n
    return jnp.where(place < n // 2, 2 * place, 2 * (n - 1 - place) + 1)


def remote(src, dst, send, recv, axis, target):
    return pltpu.make_async_remote_copy(
        src_ref=src,
        dst_ref=dst,
        send_sem=send,
        recv_sem=recv,
        device_id={axis: target},
        device_id_type=MESH,
    )


def rotation_tables(spans, span_len):
    half = HEAD_DIM // 2
    frequency = ROPE_BASE ** (-2.0 * np.arange(half, dtype=np.float64) / HEAD_DIM)
    frequency = np.concatenate([frequency, frequency])

    def table(at):
        angle = at.astype(np.float64)[:, None] * frequency[None, :]
        return np.stack([np.cos(angle), np.sin(angle)]).astype(np.float32)

    return table(np.arange(spans) * span_len), table(np.arange(span_len))


class Task:
    def __init__(self, name, rank, cost, needs=(), waits=(), sends=()):
        self.name, self.rank, self.cost = name, rank, cost
        self.needs, self.waits, self.sends = needs, waits, sends


def arrange(tasks, latency):
    now, free, arrival, done, order = 0.0, {}, {}, set(), []
    left = list(tasks)
    while left:
        best = None
        for task in left:
            if all(name in done for name in task.needs) and all(key in arrival for key in task.waits):
                at = max([arrival[key] for key in task.waits], default=0.0)
                key = (max(at, now), task.rank)
                if best is None or key < best[0]:
                    best = (key, task)
        (at, _), task = best
        left.remove(task)
        now = at + task.cost
        done.add(task.name)
        order.append(task.name)
        for key, link, cost in task.sends:
            free[link] = max(free.get(link, 0.0), now) + cost
            arrival[key] = free[link] + latency
    return order


def centred(offset, n):
    return offset + n if offset <= -(n // 2) else offset


def hops(n, d, parity):
    return n // 2 if d == parity else n // 2 - 1


GATES = (None, None, 2, 3)
LATENCY = 2.4
MESSAGE = 0.7
ATTEND = 1.02


def plan(n, m, seqs, heads):
    units = PARTS * seqs
    tasks = []

    def task(*args, **rest):
        tasks.append(Task(*args, **rest))

    def both(name, parity):
        return [(*name, d, hops(n, d, parity) - 1) for d in range(2)]

    steps = [(s, d) for s in range(n // 2) for d in range(2)]
    for u in range(units):
        gate = GATES[u // seqs]
        for s, d in steps:
            if s < hops(n, d, u % 2):
                needs = []
                if s == 0:
                    needs = [("A", v, d, 0) for v in range(u)]
                    if gate is not None:
                        needs.append(("A", 0, 0, gate))
                task(
                    ("A", u, d, s),
                    s,
                    0.01,
                    needs=needs,
                    waits=[("A", u, d, s - 1)] if s else [],
                    sends=[(("A", u, d, s), d, MESSAGE)],
                )
    task(
        ("X",),
        0.9,
        0.15,
        needs=[("A", u, d, 0) for u in range(seqs) for d in range(2)],
        sends=[(("X", o), "x", 4 * PARTS * MESSAGE / 2) for o in range(1, m)],
    )
    task(("mask",), 40, 0.2)
    task(
        ("xwait",),
        45,
        0.01,
        waits=[("X", o) for o in range(1, m)],
        needs=[("attend", 2 * seqs - 1, heads - 1)],
    )
    for c in range(seqs):
        task(("xt", c), 50 + c, 0.2, needs=[("xwait",)])
    for u in range(units):
        for k in range(heads):
            task(
                ("attend", u, k),
                20 + u + k / heads,
                ATTEND,
                needs=[("mask",)] if k == 0 else [("attend", u, k - 1)],
                waits=both(("A", u), u % 2) if k == 0 else [],
            )
        for s, d in steps:
            if s < hops(n, d, u % 2):
                task(
                    ("R", u, d, s),
                    2 + s,
                    0.03,
                    needs=[] if s else [("attend", u, heads - 1)],
                    waits=[("R", u, d, s - 1)] if s else [],
                    sends=[(("R", u, d, s), d, MESSAGE)],
                )
        task(
            ("total", u),
            4 + u / units,
            0.11,
            waits=both(("R", u), u % 2),
            sends=[(("G", u, o), "x" if o > 1 else "chip", MESSAGE) for o in range(1, m)],
        )
        task(("gwait", u), 10, 0.01, waits=[("G", u, o) for o in range(1, m)])
        task(("drain", u), 90, 0.05, needs=[("attend", units - 1, heads - 1), ("gwait", u)])
    offsets = sorted(range(-(n // 2) + 1, n // 2 + 1), key=lambda v: (-abs(v), v))
    for part in range(PARTS):
        mine = [part * seqs + c for c in range(seqs)]
        for i, offset in enumerate(offsets):
            task(
                ("M", part, offset),
                11 + part + i / 100,
                0.12,
                needs=[("gwait", u) for u in mine] + [("xt", c) for c in range(seqs)],
            )
        for half in range(2):
            for s, d in steps:
                if s < hops(n, d, half):
                    offset = centred((1, -1)[d] * (hops(n, d, half) - s), n)
                    task(
                        ("W", part, half, d, s),
                        5 + s,
                        0.03,
                        needs=[("M", part, offset)],
                        waits=[("W", part, half, d, s - 1)] if s else [],
                        sends=[(("W", part, half, d, s), d, MESSAGE)],
                    )
            task(
                ("wtotal", part, half),
                3,
                0.05,
                needs=[("M", part, 0)],
                waits=both(("W", part, half), half),
            )
            task(("wdrain", part, half), 91, 0.05, needs=[("wtotal", part, half)])
    for q in range(PIECES):
        before = [("total", u) for u in range(units)] + ([("project", q - 1)] if q else [])
        task(("project", q), 60 + q, 0.88, needs=before)
        task(("finish", q), 70 + q, 0.16, needs=[("project", PIECES - 1)])
    task(("gain",), 80, 0.13, needs=[("wtotal", part, half) for part in range(PARTS) for half in range(2)])
    return arrange(tasks, LATENCY)


def blocks_of(n, m, own, permuted):
    if permuted:
        return [(j * n * own, n * own, j, 0) for j in range(m)]
    return [(b * own, own, b % m, (b // m) * own) for b in range(n * m)]


def layer_kernel(
    n,
    m,
    permuted,
    span_hbm,
    start_hbm,
    offset_hbm,
    gain_hbm,
    rows_hbm,
    x_hbm,
    wk_hbm,
    wv_hbm,
    q_hbm,
    g_hbm,
    att,
    dq,
    gx,
    gkw,
    gvw,
    gain_out,
    span_ref,
    start_ref,
    offset_ref,
    gain_ref,
    gain_rows,
    x_ref,
    wk,
    wv,
    q_ref,
    g_ref,
    normed,
    xg,
    xt,
    kv,
    terms,
    inbox,
    gall,
    own_k,
    own_v,
    part2,
    mine,
    inbox2,
    rms_ref,
    ng,
    cos_ref,
    sin_ref,
    bias,
    ssem,
    xsem,
    wsem,
    qsem,
    a_send,
    a_recv,
    r_send,
    r_recv,
    w_send,
    w_recv,
    x_send,
    x_recv,
    g_send,
    g_recv,
):
    me = lax.axis_index("ctx")
    dp = lax.axis_index("dp")
    place = ring_place(me, n)
    sign = (1, -1)
    targets = [ring_index(place + 1, n), ring_index(place - 1, n)]
    seqs, rows, _ = q_ref.shape
    kv_width = wk.shape[1]
    model_width = x_ref.shape[2]
    count = seqs * rows
    own = gkw.shape[0]
    head = HEAD_DIM
    span_len = rows // 2
    width = kv_width // PARTS
    heads = width // head
    group = q_ref.shape[2] // kv_width
    scale = head ** (-0.5)
    units = PARTS * seqs
    half_own = own // 2
    nt = (((1,), (1,)), ((), ()))
    nn = (((1,), (0,)), ((), ()))
    tn = (((0,), (0,)), ((), ()))
    dot = functools.partial(lax.dot_general, preferred_element_type=F32)
    blocks = blocks_of(n, m, own, permuted)
    per_piece = len(blocks) // PIECES
    piece_width = model_width // PIECES

    def start(loads):
        for load in loads:
            load.start()
        return loads

    x_loads = start([pltpu.make_async_copy(x_hbm.at[c], x_ref.at[c], xsem.at[c]) for c in range(seqs)])
    small = (
        (gain_hbm, gain_ref),
        (span_hbm, span_ref),
        (start_hbm, start_ref),
        (offset_hbm, offset_ref),
        (rows_hbm, gain_rows),
    )
    small_loads = start([pltpu.make_async_copy(src, dst, ssem.at[i]) for i, (src, dst) in enumerate(small)])
    w_loads = []
    for q in range(PIECES):
        at = pl.ds(q * piece_width, piece_width)
        w_loads.append(
            [
                pltpu.make_async_copy(src.at[at], dst.at[at], wsem.at[t, q])
                for t, (src, dst) in enumerate(((wk_hbm, wk), (wv_hbm, wv)))
            ]
        )
    q_loads = [
        pltpu.make_async_copy(src, dst, qsem.at[t])
        for t, (src, dst) in enumerate(((q_hbm, q_ref), (g_hbm, g_ref)))
    ]
    start(w_loads[0])
    barrier = pltpu.get_barrier_semaphore()
    for axis, target in [("ctx", targets[0]), ("ctx", targets[1])] + [("dp", (dp + o) % m) for o in range(1, m)]:
        pl.semaphore_signal(barrier, inc=1, device_id={axis: target}, device_id_type=MESH)

    for c in range(seqs):
        x_loads[c].wait()
        if c == 0:
            for loads in w_loads[1:]:
                start(loads)
            start(q_loads)
            small_loads[0].wait()
        total = jnp.zeros((rows, 1), F32)
        for q in range(PIECES):
            wide = x_ref[c, :, q * piece_width : (q + 1) * piece_width].astype(F32)
            total = total + jnp.sum(wide * wide, axis=1, keepdims=True)
        rms = lax.rsqrt(total / model_width + EPSILON)
        rms_ref[c] = rms
        for start, size, j, offset in blocks:
            at = slice(start, start + size)
            value = (x_ref[c, :, at].astype(F32) * rms * gain_ref[:, at]).astype(BF16)
            normed[j, c, :, offset : offset + size] = value

    for load in small_loads[1:]:
        load.wait()
    offset_cos, offset_sin = offset_ref[0], offset_ref[1]
    lane = lax.broadcasted_iota(jnp.int32, (span_len, head), 1)
    signs = jnp.where(lane < head // 2, -1.0, 1.0).astype(F32)
    for half in range(2):
        span = span_ref[2 * me + half]
        start_cos = start_ref[0, pl.ds(span, 1), :]
        start_sin = start_ref[1, pl.ds(span, 1), :]
        at = slice(half * span_len, (half + 1) * span_len)
        cos_ref[at] = start_cos * offset_cos - start_sin * offset_sin
        sin_ref[at] = (start_sin * offset_cos + start_cos * offset_sin) * signs

    key = jnp.zeros((count, kv_width), F32)
    value = jnp.zeros((count, kv_width), F32)
    for q in range(PIECES):
        lhs = jnp.concatenate(
            [
                normed[j, :, :, offset : offset + size].reshape(count, size)
                for _, size, j, offset in blocks[q * per_piece : (q + 1) * per_piece]
            ],
            axis=1,
        )
        for load in w_loads[q]:
            load.wait()
        at = slice(q * piece_width, (q + 1) * piece_width)
        key = key + dot(lhs, wk[at], nn)
        value = value + dot(lhs, wv[at], nn)
    for u in range(units):
        part, c = divmod(u, seqs)
        for k in range(heads):
            col = part * width + k * head
            turn = key[c * rows : (c + 1) * rows, col : col + head]
            turned = pltpu.roll(turn, head // 2, 1)
            kv[u, me, :, k * head : (k + 1) * head] = (turn * cos_ref[...] + turned * sin_ref[...]).astype(BF16)
        kv[u, me, :, width : 2 * width] = value[
            c * rows : (c + 1) * rows, part * width : (part + 1) * width
        ].astype(BF16)
    pl.semaphore_wait(barrier, 2 + m - 1)

    def a_copy(u, d, s):
        slot = kv.at[u, ring_index(place - sign[d] * s, n)]
        return remote(slot, slot, a_send.at[u, d, s], a_recv.at[u, d, s], "ctx", targets[d])

    def a_arrive(u, d, s):
        slot = kv.at[u, ring_index(place - sign[d] * (s + 1), n)]
        remote(slot, slot, a_send.at[u, d, s], a_recv.at[u, d, s], "ctx", targets[d]).wait_recv()

    def r_copy(u, d, s):
        if s == 0:
            src = terms.at[u, ring_index(place + sign[d] * hops(n, d, u % 2), n)]
        else:
            src = inbox.at[u, d, s - 1]
        return remote(src, inbox.at[u, d, s], r_send.at[u, d, s], r_recv.at[u, d, s], "ctx", targets[d])

    def r_arrive(u, d, s):
        slot = inbox.at[u, d, s]
        remote(slot, slot, r_send.at[u, d, s], r_recv.at[u, d, s], "ctx", targets[d]).wait_recv()

    def w_copy(part, half, d, s):
        lane = 2 * part + half
        if s == 0:
            owner = ring_index(place + sign[d] * hops(n, d, half), n)
            src = part2.at[part, owner, pl.ds(half * half_own, half_own)]
        else:
            src = inbox2.at[lane, d, s - 1]
        return remote(src, inbox2.at[lane, d, s], w_send.at[lane, d, s], w_recv.at[lane, d, s], "ctx", targets[d])

    def w_arrive(part, half, d, s):
        lane = 2 * part + half
        slot = inbox2.at[lane, d, s]
        remote(slot, slot, w_send.at[lane, d, s], w_recv.at[lane, d, s], "ctx", targets[d]).wait_recv()

    def x_copy(o):
        target = (dp + o) % m
        return remote(normed.at[target], xg.at[:, dp], x_send.at[o - 1], x_recv.at[o - 1], "dp", target)

    def x_arrive(o):
        slot = xg.at[:, (dp + m - o) % m]
        remote(slot, slot, x_send.at[o - 1], x_recv.at[o - 1], "dp", (dp + o) % m).wait_recv()

    def g_copy(u, o):
        slot = gall.at[u, dp]
        return remote(slot, slot, g_send.at[u, o - 1], g_recv.at[u, o - 1], "dp", (dp + o) % m)

    def g_arrive(u, o):
        slot = gall.at[u, (dp + m - o) % m]
        remote(slot, slot, g_send.at[u, o - 1], g_recv.at[u, o - 1], "dp", (dp + o) % m).wait_recv()

    def a_step(u, d, s):
        if s > 0:
            a_arrive(u, d, s - 1)
        a_copy(u, d, s).start()

    def x_step():
        for o in range(1, m):
            x_copy(o).start()
        xg[:, dp] = normed[dp]

    def mask_step():
        for load in q_loads:
            load.wait()
        spans = 2 * n
        lane = lax.broadcasted_iota(jnp.int32, (1, n * rows), 1)
        key_pos = jnp.zeros((1, n * rows), jnp.int32)
        for k in range(spans):
            inside = (lane >= k * span_len) & (lane < (k + 1) * span_len)
            key_pos = jnp.where(inside, lane + (span_ref[k] - k) * span_len, key_pos)
        row = lax.broadcasted_iota(jnp.int32, (rows, 1), 0)
        first, second = span_ref[2 * me], span_ref[2 * me + 1]
        query_pos = row + jnp.where(row < span_len, first * span_len, (second - 1) * span_len)
        bias[...] = jnp.where(key_pos <= query_pos, 0.0, -1e30).astype(F32)

    def transpose_step(c):
        wide = xg[c].reshape(m * rows, n * own)
        xt[c] = jnp.transpose(wide).reshape(n, own, m * rows)

    def x_wait():
        for o in range(1, m):
            x_arrive(o)

    def attend_step(u, k):
        part, c = divmod(u, seqs)
        if k == 0:
            for d in range(2):
                a_arrive(u, d, hops(n, d, u % 2) - 1)
        first = ((part * heads + k) * group) * head
        columns = [slice(first + i * head, first + (i + 1) * head) for i in range(group)]
        query = jnp.concatenate([q_ref[c, :, column] for column in columns], axis=0)
        grad = jnp.concatenate([g_ref[c, :, column] for column in columns], axis=0)
        key_at = slice(k * head, (k + 1) * head)
        value_at = slice(width + k * head, width + (k + 1) * head)
        key = kv[u, :, :, key_at].reshape(n * rows, head)
        value = kv[u, :, :, value_at].reshape(n * rows, head)
        masked = jnp.concatenate([bias[...]] * group, axis=0)
        scores = dot(query, key, nt) * scale + masked
        exponent = jnp.exp(scores - jnp.max(scores, axis=1, keepdims=True))
        probability = exponent * (1.0 / jnp.sum(exponent, axis=1, keepdims=True))
        rounded = probability.astype(BF16)
        attended = dot(rounded, value, nn).astype(BF16)
        delta = jnp.sum(grad.astype(F32) * attended.astype(F32), axis=1, keepdims=True)
        dscores = (probability * (dot(grad, value, nt) - delta)).astype(BF16)
        dquery = (dot(dscores, key, nn) * scale).astype(BF16)
        for i in range(group):
            att[c, :, columns[i]] = attended[i * rows : (i + 1) * rows]
            dq[c, :, columns[i]] = dquery[i * rows : (i + 1) * rows]
        terms[u, :, :, key_at] = (dot(dscores, query, tn) * scale).astype(BF16).reshape(n, rows, head)
        terms[u, :, :, value_at] = dot(rounded, grad, tn).astype(BF16).reshape(n, rows, head)

    def r_step(u, d, s):
        if s > 0:
            r_arrive(u, d, s - 1)
            owner = ring_index(place + sign[d] * (hops(n, d, u % 2) - s), n)
            inbox[u, d, s - 1] = (inbox[u, d, s - 1].astype(F32) + terms[u, owner].astype(F32)).astype(BF16)
        r_copy(u, d, s).start()

    def r_total(u):
        part, c = divmod(u, seqs)
        result = terms[u, me].astype(F32)
        for d in (1 - u % 2, u % 2):
            last = hops(n, d, u % 2) - 1
            r_arrive(u, d, last)
            result = result + inbox[u, d, last].astype(F32)
        at = slice(c * rows, (c + 1) * rows)
        for k in range(heads):
            back = result[:, k * head : (k + 1) * head]
            turned = pltpu.roll(back, head // 2, 1)
            back = (back * cos_ref[...] - turned * sin_ref[...]).astype(BF16)
            gall[u, dp, :, k * head : (k + 1) * head] = back
            own_k[at, part * width + k * head : part * width + (k + 1) * head] = back
        back = result[:, width:].astype(BF16)
        gall[u, dp, :, width:] = back
        own_v[at, part * width : (part + 1) * width] = back
        for o in range(1, m):
            g_copy(u, o).start()

    def g_wait(u):
        for o in range(1, m):
            g_arrive(u, o)

    def product_step(part, offset):
        owner = ring_index(place + offset, n)
        total = jnp.zeros((own, 2 * width), F32)
        for c in range(seqs):
            total = total + dot(xt[c, owner], gall[part * seqs + c].reshape(m * rows, 2 * width), nn)
        if offset == 0:
            mine[part] = total
        else:
            part2[part, owner] = total.astype(BF16)

    def w_step(part, half, d, s):
        if s > 0:
            w_arrive(part, half, d, s - 1)
            lane = 2 * part + half
            owner = ring_index(place + sign[d] * (hops(n, d, half) - s), n)
            mid = part2[part, owner, half * half_own : (half + 1) * half_own]
            inbox2[lane, d, s - 1] = (inbox2[lane, d, s - 1].astype(F32) + mid.astype(F32)).astype(BF16)
        w_copy(part, half, d, s).start()

    def w_total(part, half):
        lane = 2 * part + half
        at = slice(half * half_own, (half + 1) * half_own)
        result = mine[part, at]
        for d in (1 - half, half):
            last = hops(n, d, half) - 1
            w_arrive(part, half, d, last)
            result = result + inbox2[lane, d, last].astype(F32)
        gkw[at, part * width : (part + 1) * width] = result[:, :width]
        gvw[at, part * width : (part + 1) * width] = result[:, width:]

    state = {}

    def project_step(q):
        at = slice(q * piece_width, (q + 1) * piece_width)
        piece = dot(own_k[...], wk[at], nt) + dot(own_v[...], wv[at], nt)
        ng[:, at] = piece
        wide = x_ref[:, :, at].reshape(count, piece_width).astype(F32)
        inner = jnp.sum(piece * gain_ref[:, at] * wide, axis=1, keepdims=True)
        state["inner"] = state["inner"] + inner if q else inner

    def finish_step(q):
        at = slice(q * piece_width, (q + 1) * piece_width)
        rms = rms_ref[...].reshape(count, 1)
        slope = rms * rms * rms * (state["inner"] / model_width)
        wide = x_ref[:, :, at].reshape(count, piece_width).astype(F32)
        gx[:, at] = (rms * gain_ref[:, at] * ng[:, at] - wide * slope).astype(BF16)

    def gain_step():
        block = dp * n + me if permuted else me * m + dp
        at = pl.ds(pl.multiple_of(block * own, own), own)
        both = wk[at].astype(F32) * gkw[...] + wv[at].astype(F32) * gvw[...]
        folded = both[:, :128]
        for q in range(1, kv_width // 128):
            folded = folded + both[:, q * 128 : (q + 1) * 128]
        gain_out[...] = jnp.sum(jnp.transpose(folded), axis=0, keepdims=True) / gain_rows[pl.ds(block, 1), :]

    def drain_step(u):
        for s in range(n // 2):
            for d in range(2):
                if s < hops(n, d, u % 2):
                    a_copy(u, d, s).wait_send()
                    r_copy(u, d, s).wait_send()
        for o in range(1, m):
            g_copy(u, o).wait_send()
            if u == 0:
                x_copy(o).wait_send()

    def w_drain(part, half):
        for s in range(n // 2):
            for d in range(2):
                if s < hops(n, d, half):
                    w_copy(part, half, d, s).wait_send()

    steps = {
        "A": a_step,
        "X": x_step,
        "mask": mask_step,
        "xwait": x_wait,
        "xt": transpose_step,
        "attend": attend_step,
        "R": r_step,
        "total": r_total,
        "gwait": g_wait,
        "drain": drain_step,
        "M": product_step,
        "W": w_step,
        "wtotal": w_total,
        "wdrain": w_drain,
        "project": project_step,
        "finish": finish_step,
        "gain": gain_step,
    }
    for kind, *where in plan(n, m, seqs, heads):
        steps[kind](*where)


def layer(n, m, permuted, span_order, norm_gain, tokens, key_weight, value_weight, queries, grads):
    seqs, rows, model_width = tokens.shape
    kv_width = key_weight.shape[1]
    own = model_width // (n * m)
    width = kv_width // PARTS
    units = PARTS * seqs
    count = seqs * rows
    starts, offsets = rotation_tables(2 * n, rows // 2)
    dma = pltpu.SemaphoreType.DMA
    out_shape = (
        jax.ShapeDtypeStruct(queries.shape, BF16),
        jax.ShapeDtypeStruct(queries.shape, BF16),
        jax.ShapeDtypeStruct((count, model_width), BF16),
        jax.ShapeDtypeStruct((own, kv_width), F32),
        jax.ShapeDtypeStruct((own, kv_width), F32),
        jax.ShapeDtypeStruct((1, own), F32),
    )
    vectors = [
        ((1, model_width), F32),
        ((n * m, own), F32),
        (tokens.shape, BF16),
        (key_weight.shape, BF16),
        (value_weight.shape, BF16),
        (queries.shape, BF16),
        (queries.shape, BF16),
        ((m, seqs, rows, n * own), BF16),
        ((seqs, m, rows, n * own), BF16),
        ((seqs, n, own, m * rows), BF16),
        ((units, n, rows, 2 * width), BF16),
        ((units, n, rows, 2 * width), BF16),
        ((units, 2, n // 2, rows, 2 * width), BF16),
        ((units, m, rows, 2 * width), BF16),
        ((count, kv_width), BF16),
        ((count, kv_width), BF16),
        ((PARTS, n, own, 2 * width), BF16),
        ((PARTS, own, 2 * width), F32),
        ((2 * PARTS, 2, n // 2, own // 2, 2 * width), BF16),
        ((seqs, rows, 1), F32),
        ((count, model_width), F32),
        ((rows, HEAD_DIM), F32),
        ((rows, HEAD_DIM), F32),
        ((rows, n * rows), F32),
    ]
    held = sum(int(np.prod(shape)) * jnp.dtype(kind).itemsize for shape, kind in vectors)
    limit = min(60 * MIB, held + 8 * MIB)
    ring = dma((units, 2, n // 2))
    lanes = dma((2 * PARTS, 2, n // 2))
    return pl.pallas_call(
        functools.partial(layer_kernel, n, m, permuted),
        out_shape=out_shape,
        in_specs=[HBM] * 10,
        out_specs=[VMEM] * 6,
        scratch_shapes=[
            pltpu.SMEM(span_order.shape, jnp.int32),
            pltpu.VMEM(starts.shape, F32),
            pltpu.VMEM(offsets.shape, F32),
            *[pltpu.VMEM(*spec) for spec in vectors],
            dma((5,)),
            dma((seqs,)),
            dma((2, PIECES)),
            dma((2,)),
            ring,
            ring,
            ring,
            ring,
            lanes,
            lanes,
            dma((m - 1,)),
            dma((m - 1,)),
            dma((units, m - 1)),
            dma((units, m - 1)),
        ],
        compiler_params=pltpu.CompilerParams(
            collective_id=0, has_side_effects=True, vmem_limit_bytes=limit
        ),
        name="layer",
    )(
        *[
            pltpu.with_memory_space_constraint(array, pltpu.HBM)
            for array in (
                span_order,
                jnp.asarray(starts),
                jnp.asarray(offsets),
                norm_gain[None, :],
                norm_gain.reshape(n * m, own),
                tokens,
                key_weight,
                value_weight,
                queries,
                grads,
            )
        ]
    )


def deliver_kernel(*refs):
    count = (len(refs) - 1) // 2
    sems = refs[-1]
    copies = [pltpu.make_async_copy(refs[i], refs[count + i], sems.at[i]) for i in range(count)]
    for copy in copies:
        copy.start()
    for copy in copies:
        copy.wait()


def deliver(*arrays):
    return pl.pallas_call(
        deliver_kernel,
        out_shape=tuple(jax.ShapeDtypeStruct(a.shape, a.dtype) for a in arrays),
        in_specs=[VMEM] * len(arrays),
        out_specs=[ANY] * len(arrays),
        scratch_shapes=[pltpu.SemaphoreType.DMA((len(arrays),))],
        compiler_params=pltpu.CompilerParams(vmem_limit_bytes=16 * MIB),
        name="deliver",
    )(*arrays)


def body(n, m, tokens, queries, d_attended, span_order, norm_gain, key_weight, value_weight):
    seqs, rows, model_width = tokens.shape
    own = model_width // (n * m)
    permuted = own % 128 != 0

    def shuffle(array, axis):
        shape = array.shape
        split = array.reshape(shape[:axis] + (n, m, own) + shape[axis + 1 :])
        return jnp.swapaxes(split, axis, axis + 1).reshape(shape)

    if permuted:
        tokens, norm_gain = shuffle(tokens, 2), shuffle(norm_gain, 0)
        key_weight, value_weight = shuffle(key_weight, 0), shuffle(value_weight, 0)
    attended, dquery, grad_rows, key_grad, value_grad, gain = deliver(
        *layer(n, m, permuted, span_order, norm_gain, tokens, key_weight, value_weight, queries, d_attended)
    )
    grad_rows = grad_rows.reshape(seqs, rows, model_width)
    if permuted:
        split = grad_rows.reshape(seqs, rows, m, n, own)
        grad_rows = jnp.swapaxes(split, 2, 3).reshape(seqs, rows, model_width)
    return attended, dquery, grad_rows, key_grad, value_grad, gain.reshape(own)


def solution(mesh):
    split = P("dp", "ctx", None)
    return jax.shard_map(
        functools.partial(body, mesh.shape["ctx"], mesh.shape["dp"]),
        mesh=mesh,
        in_specs=(split, split, split, P(), P(), P(), P()),
        out_specs=(
            split,
            split,
            split,
            P(("ctx", "dp"), None),
            P(("ctx", "dp"), None),
            P(("ctx", "dp")),
        ),
        check_vma=False,
    )
```

```python
import functools

import jax
import jax.numpy as jnp
import numpy as np
from jax import lax
from jax.experimental import pallas as pl
from jax.experimental.pallas import tpu as pltpu
from jax.sharding import PartitionSpec as P

HEAD_DIM = 128
ROPE_BASE = 500000.0
EPSILON = 1e-05
MESH = pl.DeviceIdType.MESH
VMEM = pl.BlockSpec(memory_space=pltpu.VMEM)
HBM = pl.BlockSpec(memory_space=pltpu.HBM)
ANY = pl.BlockSpec(memory_space=pl.ANY)
F32 = jnp.float32
BF16 = jnp.bfloat16
MIB = 1024 * 1024

PARTS = 4
PIECES = 4


def ring_place(index, n):
    return jnp.where(index % 2 == 0, index // 2, n - 1 - index // 2)


def ring_index(place, n):
    place = (place + 2 * n) % n
    return jnp.where(place < n // 2, 2 * place, 2 * (n - 1 - place) + 1)


def remote(src, dst, send, recv, axis, target):
    return pltpu.make_async_remote_copy(
        src_ref=src,
        dst_ref=dst,
        send_sem=send,
        recv_sem=recv,
        device_id={axis: target},
        device_id_type=MESH,
    )


def rotation_tables(spans, span_len):
    half = HEAD_DIM // 2
    frequency = ROPE_BASE ** (-2.0 * np.arange(half, dtype=np.float64) / HEAD_DIM)
    frequency = np.concatenate([frequency, frequency])

    def table(at):
        angle = at.astype(np.float64)[:, None] * frequency[None, :]
        return np.stack([np.cos(angle), np.sin(angle)]).astype(np.float32)

    return table(np.arange(spans) * span_len), table(np.arange(span_len))


class Task:
    def __init__(self, name, rank, cost, needs=(), waits=(), sends=()):
        self.name, self.rank, self.cost = name, rank, cost
        self.needs, self.waits, self.sends = needs, waits, sends


def arrange(tasks, latency):
    now, free, arrival, done, order = 0.0, {}, {}, set(), []
    left = list(tasks)
    while left:
        best = None
        for task in left:
            if all(name in done for name in task.needs) and all(key in arrival for key in task.waits):
                at = max([arrival[key] for key in task.waits], default=0.0)
                key = (max(at, now), task.rank)
                if best is None or key < best[0]:
                    best = (key, task)
        (at, _), task = best
        left.remove(task)
        now = at + task.cost
        done.add(task.name)
        order.append(task.name)
        for key, link, cost in task.sends:
            free[link] = max(free.get(link, 0.0), now) + cost
            arrival[key] = free[link] + latency
    return order


def hops(n, d, parity):
    return n // 2 if d == parity else n // 2 - 1


GATES = (None, None, 2, 3)
LATENCY = 2.4
MESSAGE = 0.7
ATTEND = 1.02


def plan(n, m, seqs, heads):
    units = PARTS * seqs
    tasks = []

    def task(*args, **rest):
        tasks.append(Task(*args, **rest))

    def ways(parity, s):
        return [d for d in range(2) if s < hops(n, d, parity)]

    def ring(name, parity, rank, first):
        for s in range(n // 2):
            task(
                (*name, s),
                rank + s,
                0.03,
                needs=first if s == 0 else [],
                waits=[(*name, s - 1, d) for d in ways(parity, s - 1)] if s else [],
                sends=[((*name, s, d), d, MESSAGE) for d in ways(parity, s)],
            )

    def end(name, parity):
        return [(*name, n // 2 - 1, d) for d in ways(parity, n // 2 - 1)]

    for part in range(PARTS):
        task(("proj", part), 0.5, 0.6, needs=[("proj", part - 1)] if part else [])
        for c in range(seqs):
            u = part * seqs + c
            first = [("proj", part)] + ([("A", u - 1, 0)] if u else [])
            if GATES[part] is not None:
                first.append(("A", 0, GATES[part]))
            ring(("A", u), u % 2, 0, first)
    task(
        ("X",),
        0.4,
        0.15,
        needs=[("A", seqs - 1, 0)],
        sends=[(("X", o), "x", 4 * PARTS * MESSAGE / 2) for o in range(1, m)],
    )
    task(("mask",), 40, 0.1, needs=[("proj", PARTS - 1)])
    task(
        ("xwait",),
        45,
        0.01,
        waits=[("X", o) for o in range(1, m)],
        needs=[("attend", 2 * seqs - 1, heads - 1)],
    )
    for c in range(seqs):
        task(("xt", c), 50 + c, 0.2, needs=[("xwait",)])
    for u in range(units):
        for k in range(heads):
            task(
                ("attend", u, k),
                20 + u + k / heads,
                ATTEND,
                needs=[("mask",)] if k == 0 else [("attend", u, k - 1)],
                waits=end(("A", u), u % 2) if k == 0 else [],
            )
        ring(("R", u), u % 2, 2, [("attend", u, heads - 1)])
        task(
            ("total", u),
            4 + u / units,
            0.1,
            waits=end(("R", u), u % 2),
            sends=[(("G", u, o), "x" if o > 1 else "chip", MESSAGE) for o in range(1, m)],
        )
    for part in range(PARTS):
        mine = [part * seqs + c for c in range(seqs)]
        task(
            ("M", part),
            11 + part,
            0.45,
            needs=[("xt", c) for c in range(seqs)],
            waits=[("G", u, o) for u in mine for o in range(1, m)],
        )
        for half in range(2):
            ring(("W", part, half), half, 5, [("M", part)])
            task(("wtotal", part, half), 3, 0.05, waits=end(("W", part, half), half))
        for half in range(2):
            before = [("total", u) for u in mine] + ([("project", part - 1, half)] if part else [])
            task(("project", part, half), 60 + part + half / 2, 0.55, needs=before)
    projected = [("project", part, half) for part in range(PARTS) for half in range(2)]
    for q in range(PIECES):
        before = projected if q == 0 else [("inner", q - 1)]
        task(("inner", q), 70 + q, 0.2, needs=before)
        task(("finish", q), 80 + q, 0.17, needs=[("inner", PIECES - 1)])
    task(("gain",), 90, 0.13, needs=[("wtotal", part, half) for part in range(PARTS) for half in range(2)])
    task(("drain",), 99, 0.05, needs=[("gain",)] + [("finish", q) for q in range(PIECES)])
    return arrange(tasks, LATENCY)


def blocks_of(n, m, own, permuted):
    if permuted:
        return [(j * n * own, n * own, j, 0) for j in range(m)]
    return [(b * own, own, b % m, (b // m) * own) for b in range(n * m)]


def layer_kernel(
    n,
    m,
    permuted,
    span_hbm,
    start_hbm,
    offset_hbm,
    gain_hbm,
    rows_hbm,
    x_hbm,
    wk_hbm,
    wv_hbm,
    q_hbm,
    g_hbm,
    att,
    dq,
    gx,
    gkw,
    gvw,
    gain_out,
    span_ref,
    start_ref,
    offset_ref,
    gain_ref,
    gain_rows,
    x_ref,
    wkv,
    q_ref,
    g_ref,
    normed,
    xg,
    xt,
    kv,
    terms,
    inbox,
    gall,
    own_kv,
    part2,
    inbox2,
    rms_ref,
    ng,
    cos_ref,
    sin_ref,
    bias,
    ssem,
    xsem,
    wsem,
    qsem,
    sent,
    a_recv,
    r_recv,
    w_recv,
    x_recv,
    g_recv,
):
    me = lax.axis_index("ctx")
    dp = lax.axis_index("dp")
    place = ring_place(me, n)
    sign = (1, -1)
    targets = [ring_index(place + 1, n), ring_index(place - 1, n)]
    seqs, rows, _ = q_ref.shape
    kv_width = gkw.shape[1]
    model_width = x_ref.shape[2]
    count = seqs * rows
    own = gkw.shape[0]
    head = HEAD_DIM
    span_len = rows // 2
    width = kv_width // PARTS
    heads = width // head
    group = q_ref.shape[2] // kv_width
    scale = head ** (-0.5)
    units = PARTS * seqs
    half_own = own // 2
    nt = (((1,), (1,)), ((), ()))
    nn = (((1,), (0,)), ((), ()))
    tn = (((0,), (0,)), ((), ()))
    dot = functools.partial(lax.dot_general, preferred_element_type=F32)
    blocks = blocks_of(n, m, own, permuted)
    per_piece = len(blocks) // PIECES
    piece_width = model_width // PIECES

    def start(loads):
        for load in loads:
            load.start()
        return loads

    x_loads = start([pltpu.make_async_copy(x_hbm.at[c], x_ref.at[c], xsem.at[c]) for c in range(seqs)])
    small = (
        (gain_hbm, gain_ref),
        (span_hbm, span_ref),
        (start_hbm, start_ref),
        (offset_hbm, offset_ref),
        (rows_hbm, gain_rows),
    )
    small_loads = start([pltpu.make_async_copy(src, dst, ssem.at[i]) for i, (src, dst) in enumerate(small)])
    w_loads = [
        [
            pltpu.make_async_copy(
                src.at[:, pl.ds(part * width, width)], wkv.at[part, :, pl.ds(t * width, width)], wsem.at[part]
            )
            for t, src in enumerate((wk_hbm, wv_hbm))
        ]
        for part in range(PARTS)
    ]
    q_loads = [
        pltpu.make_async_copy(src, dst, qsem.at[t])
        for t, (src, dst) in enumerate(((q_hbm, q_ref), (g_hbm, g_ref)))
    ]
    start(w_loads[0])
    barrier = pltpu.get_barrier_semaphore()
    for axis, target in [("ctx", targets[0]), ("ctx", targets[1])] + [("dp", (dp + o) % m) for o in range(1, m)]:
        pl.semaphore_signal(barrier, inc=1, device_id={axis: target}, device_id_type=MESH)

    for c in range(seqs):
        x_loads[c].wait()
        if c == 0:
            for loads in w_loads[1:]:
                start(loads)
            start(q_loads)
            small_loads[0].wait()
        total = jnp.zeros((rows, 1), F32)
        for q in range(PIECES):
            wide = x_ref[c, :, q * piece_width : (q + 1) * piece_width].astype(F32)
            total = total + jnp.sum(wide * wide, axis=1, keepdims=True)
        rms = lax.rsqrt(total / model_width + EPSILON)
        rms_ref[c] = rms
        for start, size, j, offset in blocks:
            at = slice(start, start + size)
            value = (x_ref[c, :, at].astype(F32) * rms * gain_ref[:, at]).astype(BF16)
            normed[j, c, :, offset : offset + size] = value

    for load in small_loads[1:]:
        load.wait()
    offset_cos, offset_sin = offset_ref[0], offset_ref[1]
    lane = lax.broadcasted_iota(jnp.int32, (span_len, head), 1)
    signs = jnp.where(lane < head // 2, -1.0, 1.0).astype(F32)
    for half in range(2):
        span = span_ref[2 * me + half]
        start_cos = start_ref[0, pl.ds(span, 1), :]
        start_sin = start_ref[1, pl.ds(span, 1), :]
        at = slice(half * span_len, (half + 1) * span_len)
        cos_ref[at] = start_cos * offset_cos - start_sin * offset_sin
        sin_ref[at] = (start_sin * offset_cos + start_cos * offset_sin) * signs

    def proj_step(part):
        pltpu.make_async_copy(wkv.at[part], wkv.at[part], wsem.at[part]).wait()
        both = jnp.zeros((count, 2 * width), F32)
        for q in range(PIECES):
            lhs = jnp.concatenate(
                [
                    normed[j, :, :, offset : offset + size].reshape(count, size)
                    for _, size, j, offset in blocks[q * per_piece : (q + 1) * per_piece]
                ],
                axis=1,
            )
            both = both + dot(lhs, wkv[part, q * piece_width : (q + 1) * piece_width], nn)
        for c in range(seqs):
            u = part * seqs + c
            at = slice(c * rows, (c + 1) * rows)
            for k in range(heads):
                turn = both[at, k * head : (k + 1) * head]
                turned = pltpu.roll(turn, head // 2, 1)
                kv[u, me, :, k * head : (k + 1) * head] = (turn * cos_ref[...] + turned * sin_ref[...]).astype(BF16)
            kv[u, me, :, width : 2 * width] = both[at, width:].astype(BF16)
        if part == 0:
            pl.semaphore_wait(barrier, 2 + m - 1)

    def ways(parity, s):
        return [d for d in range(2) if s < hops(n, d, parity)]

    def arrive(ref, send, recv):
        remote(ref, ref, send, recv, "ctx", targets[0]).wait_recv()

    def send_on(src, dst, sends, recv, d):
        remote(src, dst, sends, recv, "ctx", targets[d]).start()

    def a_arrive(u, s):
        arrive(kv.at[u, pl.ds(0, len(ways(u % 2, s)))], sent.at[0], a_recv.at[u, s])

    def a_step(u, s):
        if s > 0:
            a_arrive(u, s - 1)
        for d in ways(u % 2, s):
            slot = kv.at[u, ring_index(place - sign[d] * s, n)]
            send_on(slot, slot, sent.at[0], a_recv.at[u, s], d)

    def x_step():
        for o in range(1, m):
            target = (dp + o) % m
            remote(normed.at[target], xg.at[:, dp], sent.at[3], x_recv.at[0], "dp", target).start()
        xg[:, dp] = normed[dp]

    def mask_step():
        for load in q_loads:
            load.wait()
        spans = 2 * n
        lane = lax.broadcasted_iota(jnp.int32, (1, n * rows), 1)
        key_pos = jnp.zeros((1, n * rows), jnp.int32)
        for k in range(spans):
            inside = (lane >= k * span_len) & (lane < (k + 1) * span_len)
            key_pos = jnp.where(inside, lane + (span_ref[k] - k) * span_len, key_pos)
        row = lax.broadcasted_iota(jnp.int32, (rows, 1), 0)
        first, second = span_ref[2 * me], span_ref[2 * me + 1]
        query_pos = row + jnp.where(row < span_len, first * span_len, (second - 1) * span_len)
        bias[...] = jnp.where(key_pos <= query_pos, 0.0, -1e30).astype(F32)

    def transpose_step(c):
        wide = xg[c].reshape(m * rows, n * own)
        xt[:, c * m * rows : (c + 1) * m * rows] = jnp.transpose(wide)

    def x_wait():
        slots = xg.at[:, pl.ds(0, m - 1)]
        remote(slots, slots, sent.at[3], x_recv.at[0], "dp", (dp + 1) % m).wait_recv()

    def attend_step(u, k):
        part, c = divmod(u, seqs)
        if k == 0:
            a_arrive(u, n // 2 - 1)
        first = ((part * heads + k) * group) * head
        columns = [slice(first + i * head, first + (i + 1) * head) for i in range(group)]
        query = jnp.concatenate([q_ref[c, :, column] for column in columns], axis=0)
        grad = jnp.concatenate([g_ref[c, :, column] for column in columns], axis=0)
        key_at = slice(k * head, (k + 1) * head)
        value_at = slice(width + k * head, width + (k + 1) * head)
        key = kv[u, :, :, key_at].reshape(n * rows, head)
        value = kv[u, :, :, value_at].reshape(n * rows, head)
        masked = jnp.concatenate([bias[...]] * group, axis=0)
        scores = dot(query, key, nt) * scale + masked
        exponent = jnp.exp(scores - jnp.max(scores, axis=1, keepdims=True))
        probability = exponent * (1.0 / jnp.sum(exponent, axis=1, keepdims=True))
        rounded = probability.astype(BF16)
        attended = dot(rounded, value, nn).astype(BF16)
        delta = jnp.sum(grad.astype(F32) * attended.astype(F32), axis=1, keepdims=True)
        dscores = (probability * (dot(grad, value, nt) - delta)).astype(BF16)
        dquery = (dot(dscores, key, nn) * scale).astype(BF16)
        for i in range(group):
            att[c, :, columns[i]] = attended[i * rows : (i + 1) * rows]
            dq[c, :, columns[i]] = dquery[i * rows : (i + 1) * rows]
        terms[u, :, :, key_at] = (dot(dscores, query, tn) * scale).astype(BF16).reshape(n, rows, head)
        terms[u, :, :, value_at] = dot(rounded, grad, tn).astype(BF16).reshape(n, rows, head)

    def r_arrive(u, s):
        d = ways(u % 2, s)
        arrive(inbox.at[u, pl.ds(d[0], len(d)), s], sent.at[1], r_recv.at[u, s])

    def r_step(u, s):
        if s > 0:
            r_arrive(u, s - 1)
        for d in ways(u % 2, s):
            owner = ring_index(place + sign[d] * (hops(n, d, u % 2) - s), n)
            src = terms.at[u, owner]
            if s > 0:
                src = inbox.at[u, d, s - 1]
                src[...] = (src[...].astype(F32) + terms[u, owner].astype(F32)).astype(BF16)
            send_on(src, inbox.at[u, d, s], sent.at[1], r_recv.at[u, s], d)

    def r_total(u):
        part, c = divmod(u, seqs)
        r_arrive(u, n // 2 - 1)
        result = terms[u, me].astype(F32)
        for d in (1 - u % 2, u % 2):
            result = result + inbox[u, d, hops(n, d, u % 2) - 1].astype(F32)
        at = slice(c * rows, (c + 1) * rows)
        for k in range(heads):
            back = result[:, k * head : (k + 1) * head]
            turned = pltpu.roll(back, head // 2, 1)
            back = (back * cos_ref[...] - turned * sin_ref[...]).astype(BF16)
            gall[u, dp, :, k * head : (k + 1) * head] = back
            own_kv[part, at, k * head : (k + 1) * head] = back
        back = result[:, width:].astype(BF16)
        gall[u, dp, :, width:] = back
        own_kv[part, at, width:] = back
        for o in range(1, m):
            slot = gall.at[u, dp]
            remote(slot, slot, sent.at[4], g_recv.at[part], "dp", (dp + o) % m).start()

    def product_step(part):
        slots = gall.at[pl.ds(part * seqs, seqs), pl.ds(0, m - 1)]
        remote(slots, slots, sent.at[4], g_recv.at[part], "dp", (dp + 1) % m).wait_recv()
        grads = gall[part * seqs : (part + 1) * seqs].reshape(seqs * m * rows, 2 * width)
        part2[part] = dot(xt[...], grads, nn).astype(BF16).reshape(n, own, 2 * width)

    def w_arrive(lane, half, s):
        d = ways(half, s)
        arrive(inbox2.at[lane, pl.ds(d[0], len(d)), s], sent.at[2], w_recv.at[lane, s])

    def w_step(part, half, s):
        lane = 2 * part + half
        if s > 0:
            w_arrive(lane, half, s - 1)
        for d in ways(half, s):
            owner = ring_index(place + sign[d] * (hops(n, d, half) - s), n)
            at = pl.ds(half * half_own, half_own)
            src = part2.at[part, owner, at]
            if s > 0:
                src = inbox2.at[lane, d, s - 1]
                src[...] = (src[...].astype(F32) + part2[part, owner, at].astype(F32)).astype(BF16)
            send_on(src, inbox2.at[lane, d, s], sent.at[2], w_recv.at[lane, s], d)

    def w_total(part, half):
        lane = 2 * part + half
        w_arrive(lane, half, n // 2 - 1)
        at = slice(half * half_own, (half + 1) * half_own)
        result = part2[part, me, at].astype(F32)
        for d in (1 - half, half):
            result = result + inbox2[lane, d, hops(n, d, half) - 1].astype(F32)
        gkw[at, part * width : (part + 1) * width] = result[:, :width]
        gvw[at, part * width : (part + 1) * width] = result[:, width:]

    state = {}

    def project_step(part, half):
        at = slice(half * model_width // 2, (half + 1) * model_width // 2)
        piece = dot(own_kv[part], wkv[part, at], nt)
        ng[:, at] = ng[:, at] + piece if part else piece

    def inner_step(q):
        at = slice(q * piece_width, (q + 1) * piece_width)
        wide = x_ref[:, :, at].reshape(count, piece_width).astype(F32)
        inner = jnp.sum(ng[:, at] * gain_ref[:, at] * wide, axis=1, keepdims=True)
        state["inner"] = state["inner"] + inner if q else inner

    def finish_step(q):
        at = slice(q * piece_width, (q + 1) * piece_width)
        rms = rms_ref[...].reshape(count, 1)
        slope = rms * rms * rms * (state["inner"] / model_width)
        wide = x_ref[:, :, at].reshape(count, piece_width).astype(F32)
        gx[:, at] = (rms * gain_ref[:, at] * ng[:, at] - wide * slope).astype(BF16)

    def gain_step():
        block = dp * n + me if permuted else me * m + dp
        at = pl.ds(pl.multiple_of(block * own, own), own)
        folded = jnp.zeros((own, width), F32)
        for part in range(PARTS):
            columns = slice(part * width, (part + 1) * width)
            folded = folded + wkv[part, at, :width].astype(F32) * gkw[:, columns]
            folded = folded + wkv[part, at, width:].astype(F32) * gvw[:, columns]
        gain_out[...] = jnp.sum(jnp.transpose(folded), axis=0, keepdims=True) / gain_rows[pl.ds(block, 1), :]

    def drain_step():
        rings = kv.at[:, pl.ds(0, n - 1)]
        lanes = part2.at[:, pl.ds(0, n - 1)]
        slices = xg.at[:, pl.ds(0, m - 1)]
        grads = gall.at[:, pl.ds(0, m - 1)]
        for i, ref in enumerate((rings, rings, lanes, slices, grads)):
            remote(ref, ref, sent.at[i], x_recv.at[0], "ctx", targets[0]).wait_send()

    steps = {
        "proj": proj_step,
        "A": a_step,
        "X": x_step,
        "mask": mask_step,
        "xwait": x_wait,
        "xt": transpose_step,
        "attend": attend_step,
        "R": r_step,
        "total": r_total,
        "drain": drain_step,
        "M": product_step,
        "W": w_step,
        "wtotal": w_total,
        "project": project_step,
        "inner": inner_step,
        "finish": finish_step,
        "gain": gain_step,
    }
    for kind, *where in plan(n, m, seqs, heads):
        steps[kind](*where)


def layer(n, m, permuted, span_order, norm_gain, tokens, key_weight, value_weight, queries, grads):
    seqs, rows, model_width = tokens.shape
    kv_width = key_weight.shape[1]
    own = model_width // (n * m)
    width = kv_width // PARTS
    units = PARTS * seqs
    count = seqs * rows
    starts, offsets = rotation_tables(2 * n, rows // 2)
    dma = pltpu.SemaphoreType.DMA
    out_shape = (
        jax.ShapeDtypeStruct(queries.shape, BF16),
        jax.ShapeDtypeStruct(queries.shape, BF16),
        jax.ShapeDtypeStruct((count, model_width), BF16),
        jax.ShapeDtypeStruct((own, kv_width), F32),
        jax.ShapeDtypeStruct((own, kv_width), F32),
        jax.ShapeDtypeStruct((1, own), F32),
    )
    vectors = [
        ((1, model_width), F32),
        ((n * m, own), F32),
        (tokens.shape, BF16),
        ((PARTS, model_width, 2 * width), BF16),
        (queries.shape, BF16),
        (queries.shape, BF16),
        ((m, seqs, rows, n * own), BF16),
        ((seqs, m, rows, n * own), BF16),
        ((n * own, seqs * m * rows), BF16),
        ((units, n, rows, 2 * width), BF16),
        ((units, n, rows, 2 * width), BF16),
        ((units, 2, n // 2, rows, 2 * width), BF16),
        ((units, m, rows, 2 * width), BF16),
        ((PARTS, count, 2 * width), BF16),
        ((PARTS, n, own, 2 * width), BF16),
        ((2 * PARTS, 2, n // 2, own // 2, 2 * width), BF16),
        ((seqs, rows, 1), F32),
        ((count, model_width), F32),
        ((rows, HEAD_DIM), F32),
        ((rows, HEAD_DIM), F32),
        ((rows, n * rows), F32),
    ]
    held = sum(int(np.prod(shape)) * jnp.dtype(kind).itemsize for shape, kind in vectors)
    limit = min(60 * MIB, held + 8 * MIB)
    ring = dma((units, n // 2))
    return pl.pallas_call(
        functools.partial(layer_kernel, n, m, permuted),
        out_shape=out_shape,
        in_specs=[HBM] * 10,
        out_specs=[VMEM] * 6,
        scratch_shapes=[
            pltpu.SMEM(span_order.shape, jnp.int32),
            pltpu.VMEM(starts.shape, F32),
            pltpu.VMEM(offsets.shape, F32),
            *[pltpu.VMEM(*spec) for spec in vectors],
            dma((5,)),
            dma((seqs,)),
            dma((PARTS,)),
            dma((2,)),
            dma((5,)),
            ring,
            ring,
            dma((2 * PARTS, n // 2)),
            dma((1,)),
            dma((PARTS,)),
        ],
        compiler_params=pltpu.CompilerParams(
            collective_id=0, has_side_effects=True, vmem_limit_bytes=limit
        ),
        name="layer",
    )(
        *[
            pltpu.with_memory_space_constraint(array, pltpu.HBM)
            for array in (
                span_order,
                jnp.asarray(starts),
                jnp.asarray(offsets),
                norm_gain[None, :],
                norm_gain.reshape(n * m, own),
                tokens,
                key_weight,
                value_weight,
                queries,
                grads,
            )
        ]
    )


def deliver_kernel(*refs):
    count = (len(refs) - 1) // 2
    sems = refs[-1]
    copies = [pltpu.make_async_copy(refs[i], refs[count + i], sems.at[i]) for i in range(count)]
    for copy in copies:
        copy.start()
    for copy in copies:
        copy.wait()


def deliver(*arrays):
    return pl.pallas_call(
        deliver_kernel,
        out_shape=tuple(jax.ShapeDtypeStruct(a.shape, a.dtype) for a in arrays),
        in_specs=[VMEM] * len(arrays),
        out_specs=[ANY] * len(arrays),
        scratch_shapes=[pltpu.SemaphoreType.DMA((len(arrays),))],
        compiler_params=pltpu.CompilerParams(vmem_limit_bytes=16 * MIB),
        name="deliver",
    )(*arrays)


def body(n, m, tokens, queries, d_attended, span_order, norm_gain, key_weight, value_weight):
    seqs, rows, model_width = tokens.shape
    own = model_width // (n * m)
    permuted = own % 128 != 0

    def shuffle(array, axis):
        shape = array.shape
        split = array.reshape(shape[:axis] + (n, m, own) + shape[axis + 1 :])
        return jnp.swapaxes(split, axis, axis + 1).reshape(shape)

    if permuted:
        tokens, norm_gain = shuffle(tokens, 2), shuffle(norm_gain, 0)
        key_weight, value_weight = shuffle(key_weight, 0), shuffle(value_weight, 0)
    attended, dquery, grad_rows, key_grad, value_grad, gain = deliver(
        *layer(n, m, permuted, span_order, norm_gain, tokens, key_weight, value_weight, queries, d_attended)
    )
    grad_rows = grad_rows.reshape(seqs, rows, model_width)
    if permuted:
        split = grad_rows.reshape(seqs, rows, m, n, own)
        grad_rows = jnp.swapaxes(split, 2, 3).reshape(seqs, rows, model_width)
    return attended, dquery, grad_rows, key_grad, value_grad, gain.reshape(own)


def solution(mesh):
    split = P("dp", "ctx", None)
    return jax.shard_map(
        functools.partial(body, mesh.shape["ctx"], mesh.shape["dp"]),
        mesh=mesh,
        in_specs=(split, split, split, P(), P(), P(), P()),
        out_specs=(
            split,
            split,
            split,
            P(("ctx", "dp"), None),
            P(("ctx", "dp"), None),
            P(("ctx", "dp")),
        ),
        check_vma=False,
    )
```

```python
import functools

import jax
import jax.numpy as jnp
import numpy as np
from jax import lax
from jax.experimental import pallas as pl
from jax.experimental.pallas import tpu as pltpu
from jax.sharding import PartitionSpec as P

HEAD_DIM = 128
ROPE_BASE = 500000.0
EPSILON = 1e-05
MESH = pl.DeviceIdType.MESH
VMEM = pl.BlockSpec(memory_space=pltpu.VMEM)
HBM = pl.BlockSpec(memory_space=pltpu.HBM)
ANY = pl.BlockSpec(memory_space=pl.ANY)
F32 = jnp.float32
BF16 = jnp.bfloat16
MIB = 1024 * 1024

PARTS = 4
PIECES = 4


def ring_place(index, n):
    return jnp.where(index % 2 == 0, index // 2, n - 1 - index // 2)


def ring_index(place, n):
    place = (place + 2 * n) % n
    return jnp.where(place < n // 2, 2 * place, 2 * (n - 1 - place) + 1)


def remote(src, dst, send, recv, axis, target):
    return pltpu.make_async_remote_copy(
        src_ref=src,
        dst_ref=dst,
        send_sem=send,
        recv_sem=recv,
        device_id={axis: target},
        device_id_type=MESH,
    )


def rotation_tables(spans, span_len):
    half = HEAD_DIM // 2
    frequency = ROPE_BASE ** (-2.0 * np.arange(half, dtype=np.float64) / HEAD_DIM)
    frequency = np.concatenate([frequency, frequency])

    def table(at):
        angle = at.astype(np.float64)[:, None] * frequency[None, :]
        return np.stack([np.cos(angle), np.sin(angle)]).astype(np.float32)

    return table(np.arange(spans) * span_len), table(np.arange(span_len))


class Task:
    def __init__(self, name, rank, cost, needs=(), waits=(), sends=()):
        self.name, self.rank, self.cost = name, rank, cost
        self.needs, self.waits, self.sends = needs, waits, sends


def arrange(tasks, latency):
    now, free, arrival, done, order = 0.0, {}, {}, set(), []
    left = list(tasks)
    while left:
        best = None
        for task in left:
            if all(name in done for name in task.needs) and all(key in arrival for key in task.waits):
                at = max([arrival[key] for key in task.waits], default=0.0)
                key = (max(at, now), task.rank)
                if best is None or key < best[0]:
                    best = (key, task)
        (at, _), task = best
        left.remove(task)
        now = at + task.cost
        done.add(task.name)
        order.append(task.name)
        for key, link, cost in task.sends:
            free[link] = max(free.get(link, 0.0), now) + cost
            arrival[key] = free[link] + latency
    return order


def hops(n, d, parity):
    return n // 2 if d == parity else n // 2 - 1


GATES = (None, 0, 2, 3)
LATENCY = 3.1
MESSAGE = 0.7
ATTEND = 1.02


def plan(n, m, seqs, heads):
    units = PARTS * seqs
    tasks = []

    def task(*args, **rest):
        tasks.append(Task(*args, **rest))

    def ways(parity, s):
        return [d for d in range(2) if s < hops(n, d, parity)]

    def ring(name, parity, rank, first):
        for s in range(n // 2):
            task(
                (*name, s),
                rank + s,
                0.03,
                needs=first if s == 0 else [],
                waits=[(*name, s - 1, d) for d in ways(parity, s - 1)] if s else [],
                sends=[((*name, s, d), d, MESSAGE) for d in ways(parity, s)],
            )

    def end(name, parity):
        return [(*name, n // 2 - 1, d) for d in ways(parity, n // 2 - 1)]

    for part in range(PARTS):
        task(("proj", part), 0.5, 0.75, needs=[("proj", part - 1)] if part else [])
        for c in range(seqs):
            u = part * seqs + c
            first = [("proj", part)] + ([("A", u - 1, 0)] if u else [])
            if GATES[part] is not None:
                first.append(("A", 0, GATES[part]))
            ring(("A", u), u % 2, 0.3 * part, first)
    task(
        ("X",),
        0.4,
        0.15,
        needs=[("A", seqs - 1, 0)],
        sends=[(("X", o), "x", 4 * PARTS * MESSAGE / 2) for o in range(1, m)],
    )
    task(("mask",), 40, 0.1, needs=[("proj", PARTS - 1)])
    task(
        ("xwait",),
        45,
        0.01,
        waits=[("X", o) for o in range(1, m)],
        needs=[("attend", 2 * seqs - 1, heads - 1)],
    )
    for c in range(seqs):
        task(("xt", c), 50 + c, 0.2, needs=[("xwait",)])
    for u in range(units):
        for k in range(heads):
            task(
                ("attend", u, k),
                20 + u + k / heads,
                ATTEND,
                needs=[("mask",)] if k == 0 else [("attend", u, k - 1)],
                waits=end(("A", u), u % 2) if k == 0 else [],
            )
        ring(("R", u), u % 2, 2 + 0.3 * (u // seqs), [("attend", u, heads - 1)])
        task(
            ("total", u),
            4 + u / units,
            0.1,
            waits=end(("R", u), u % 2),
            sends=[(("G", u, o), "x" if o > 1 else "chip", MESSAGE) for o in range(1, m)],
        )
    for part in range(PARTS):
        mine = [part * seqs + c for c in range(seqs)]
        task(
            ("M", part),
            11 + part,
            0.7,
            needs=[("xt", c) for c in range(seqs)],
            waits=[("G", u, o) for u in mine for o in range(1, m)],
        )
        for half in range(2):
            ring(("W", part, half), half, 2 + 0.3 * part, [("M", part)])
            task(("wtotal", part, half), 3, 0.05, waits=end(("W", part, half), half))
        for half in range(2):
            before = [("total", u) for u in mine] + ([("project", part - 1, half)] if part else [])
            task(("project", part, half), 60 + part + half / 2, 0.47, needs=before)
    projected = [("project", part, half) for part in range(PARTS) for half in range(2)]
    for q in range(PIECES):
        before = projected if q == 0 else [("inner", q - 1)]
        task(("inner", q), 70 + q, 0.13, needs=before)
        task(("finish", q), 80 + q, 0.17, needs=[("inner", PIECES - 1)])
    task(("gain",), 90, 0.13, needs=[("wtotal", part, half) for part in range(PARTS) for half in range(2)])
    task(("drain",), 99, 0.05, needs=[("gain",)] + [("finish", q) for q in range(PIECES)])
    return arrange(tasks, LATENCY)


def blocks_of(n, m, own, permuted):
    if permuted:
        return [(j * n * own, n * own, j, 0) for j in range(m)]
    return [(b * own, own, b % m, (b // m) * own) for b in range(n * m)]


def layer_kernel(
    n,
    m,
    permuted,
    span_hbm,
    start_hbm,
    offset_hbm,
    gain_hbm,
    rows_hbm,
    x_hbm,
    wk_hbm,
    wv_hbm,
    q_hbm,
    g_hbm,
    att,
    dq,
    gx,
    gkw,
    gvw,
    gain_out,
    span_ref,
    start_ref,
    offset_ref,
    gain_ref,
    gain_rows,
    x_ref,
    wkv,
    q_ref,
    g_ref,
    normed,
    xg,
    xt,
    kv,
    terms,
    inbox,
    gall,
    own_kv,
    part2,
    inbox2,
    rms_ref,
    ng,
    cos_ref,
    sin_ref,
    bias,
    ssem,
    xsem,
    wsem,
    qsem,
    sent,
    a_recv,
    r_recv,
    w_recv,
    x_recv,
    g_recv,
):
    me = lax.axis_index("ctx")
    dp = lax.axis_index("dp")
    place = ring_place(me, n)
    sign = (1, -1)
    targets = [ring_index(place + 1, n), ring_index(place - 1, n)]
    seqs, rows, _ = q_ref.shape
    kv_width = gkw.shape[1]
    model_width = x_ref.shape[2]
    count = seqs * rows
    own = gkw.shape[0]
    head = HEAD_DIM
    span_len = rows // 2
    width = kv_width // PARTS
    heads = width // head
    group = q_ref.shape[2] // kv_width
    scale = head ** (-0.5)
    units = PARTS * seqs
    half_own = own // 2
    nt = (((1,), (1,)), ((), ()))
    nn = (((1,), (0,)), ((), ()))
    tn = (((0,), (0,)), ((), ()))
    dot = functools.partial(lax.dot_general, preferred_element_type=F32)
    blocks = blocks_of(n, m, own, permuted)
    per_piece = len(blocks) // PIECES
    piece_width = model_width // PIECES

    def start(loads):
        for load in loads:
            load.start()
        return loads

    x_loads = start([pltpu.make_async_copy(x_hbm.at[c], x_ref.at[c], xsem.at[c]) for c in range(seqs)])
    small = (
        (gain_hbm, gain_ref),
        (span_hbm, span_ref),
        (start_hbm, start_ref),
        (offset_hbm, offset_ref),
        (rows_hbm, gain_rows),
    )
    small_loads = start([pltpu.make_async_copy(src, dst, ssem.at[i]) for i, (src, dst) in enumerate(small)])
    w_loads = [
        [
            pltpu.make_async_copy(
                src.at[:, pl.ds(part * width, width)], wkv.at[part, :, pl.ds(t * width, width)], wsem.at[part]
            )
            for t, src in enumerate((wk_hbm, wv_hbm))
        ]
        for part in range(PARTS)
    ]
    q_loads = [
        pltpu.make_async_copy(src, dst, qsem.at[t])
        for t, (src, dst) in enumerate(((q_hbm, q_ref), (g_hbm, g_ref)))
    ]
    start(w_loads[0])
    barrier = pltpu.get_barrier_semaphore()
    for axis, target in [("ctx", targets[0]), ("ctx", targets[1])] + [("dp", (dp + o) % m) for o in range(1, m)]:
        pl.semaphore_signal(barrier, inc=1, device_id={axis: target}, device_id_type=MESH)

    for c in range(seqs):
        x_loads[c].wait()
        if c == 0:
            for loads in w_loads[1:]:
                start(loads)
            start(q_loads)
            small_loads[0].wait()
        total = jnp.zeros((rows, 1), F32)
        for q in range(PIECES):
            wide = x_ref[c, :, q * piece_width : (q + 1) * piece_width].astype(F32)
            total = total + jnp.sum(wide * wide, axis=1, keepdims=True)
        rms = lax.rsqrt(total / model_width + EPSILON)
        rms_ref[c] = rms
        for start, size, j, offset in blocks:
            at = slice(start, start + size)
            value = (x_ref[c, :, at].astype(F32) * rms * gain_ref[:, at]).astype(BF16)
            normed[j, c, :, offset : offset + size] = value

    for load in small_loads[1:]:
        load.wait()
    offset_cos, offset_sin = offset_ref[0], offset_ref[1]
    lane = lax.broadcasted_iota(jnp.int32, (span_len, head), 1)
    signs = jnp.where(lane < head // 2, -1.0, 1.0).astype(F32)
    for half in range(2):
        span = span_ref[2 * me + half]
        start_cos = start_ref[0, pl.ds(span, 1), :]
        start_sin = start_ref[1, pl.ds(span, 1), :]
        at = slice(half * span_len, (half + 1) * span_len)
        cos_ref[at] = start_cos * offset_cos - start_sin * offset_sin
        sin_ref[at] = (start_sin * offset_cos + start_cos * offset_sin) * signs

    def proj_step(part):
        pltpu.make_async_copy(wkv.at[part], wkv.at[part], wsem.at[part]).wait()
        both = jnp.zeros((count, 2 * width), F32)
        for q in range(PIECES):
            lhs = jnp.concatenate(
                [
                    normed[j, :, :, offset : offset + size].reshape(count, size)
                    for _, size, j, offset in blocks[q * per_piece : (q + 1) * per_piece]
                ],
                axis=1,
            )
            both = both + dot(lhs, wkv[part, q * piece_width : (q + 1) * piece_width], nn)
        for c in range(seqs):
            u = part * seqs + c
            at = slice(c * rows, (c + 1) * rows)
            for k in range(heads):
                turn = both[at, k * head : (k + 1) * head]
                turned = pltpu.roll(turn, head // 2, 1)
                kv[u, me, :, k * head : (k + 1) * head] = (turn * cos_ref[...] + turned * sin_ref[...]).astype(BF16)
            kv[u, me, :, width : 2 * width] = both[at, width:].astype(BF16)
        if part == 0:
            pl.semaphore_wait(barrier, 2 + m - 1)

    def ways(parity, s):
        return [d for d in range(2) if s < hops(n, d, parity)]

    def arrive(ref, send, recv):
        remote(ref, ref, send, recv, "ctx", targets[0]).wait_recv()

    def send_on(src, dst, sends, recv, d):
        remote(src, dst, sends, recv, "ctx", targets[d]).start()

    def a_arrive(u, s):
        arrive(kv.at[u, pl.ds(0, len(ways(u % 2, s)))], sent.at[0], a_recv.at[u, s])

    def a_step(u, s):
        if s > 0:
            a_arrive(u, s - 1)
        for d in ways(u % 2, s):
            slot = kv.at[u, ring_index(place - sign[d] * s, n)]
            send_on(slot, slot, sent.at[0], a_recv.at[u, s], d)

    def x_step():
        for o in range(1, m):
            target = (dp + o) % m
            remote(normed.at[target], xg.at[:, dp], sent.at[3], x_recv.at[0], "dp", target).start()
        xg[:, dp] = normed[dp]

    def mask_step():
        for load in q_loads:
            load.wait()
        spans = 2 * n
        lane = lax.broadcasted_iota(jnp.int32, (1, n * rows), 1)
        key_pos = jnp.zeros((1, n * rows), jnp.int32)
        for k in range(spans):
            inside = (lane >= k * span_len) & (lane < (k + 1) * span_len)
            key_pos = jnp.where(inside, lane + (span_ref[k] - k) * span_len, key_pos)
        row = lax.broadcasted_iota(jnp.int32, (rows, 1), 0)
        first, second = span_ref[2 * me], span_ref[2 * me + 1]
        query_pos = row + jnp.where(row < span_len, first * span_len, (second - 1) * span_len)
        bias[...] = jnp.where(key_pos <= query_pos, 0.0, -1e30).astype(F32)

    def transpose_step(c):
        wide = xg[c].reshape(m * rows, n * own)
        xt[:, c * m * rows : (c + 1) * m * rows] = jnp.transpose(wide)

    def x_wait():
        slots = xg.at[:, pl.ds(0, m - 1)]
        remote(slots, slots, sent.at[3], x_recv.at[0], "dp", (dp + 1) % m).wait_recv()

    def attend_step(u, k):
        part, c = divmod(u, seqs)
        if k == 0:
            a_arrive(u, n // 2 - 1)
        first = ((part * heads + k) * group) * head
        columns = [slice(first + i * head, first + (i + 1) * head) for i in range(group)]
        query = jnp.concatenate([q_ref[c, :, column] for column in columns], axis=0)
        grad = jnp.concatenate([g_ref[c, :, column] for column in columns], axis=0)
        key_at = slice(k * head, (k + 1) * head)
        value_at = slice(width + k * head, width + (k + 1) * head)
        key = kv[u, :, :, key_at].reshape(n * rows, head)
        value = kv[u, :, :, value_at].reshape(n * rows, head)
        masked = jnp.concatenate([bias[...]] * group, axis=0)
        scores = dot(query, key, nt) * scale + masked
        exponent = jnp.exp(scores - jnp.max(scores, axis=1, keepdims=True))
        probability = exponent * (1.0 / jnp.sum(exponent, axis=1, keepdims=True))
        rounded = probability.astype(BF16)
        attended = dot(rounded, value, nn).astype(BF16)
        delta = jnp.sum(grad.astype(F32) * attended.astype(F32), axis=1, keepdims=True)
        dscores = (probability * (dot(grad, value, nt) - delta)).astype(BF16)
        dquery = (dot(dscores, key, nn) * scale).astype(BF16)
        for i in range(group):
            att[c, :, columns[i]] = attended[i * rows : (i + 1) * rows]
            dq[c, :, columns[i]] = dquery[i * rows : (i + 1) * rows]
        terms[u, :, :, key_at] = (dot(dscores, query, tn) * scale).astype(BF16).reshape(n, rows, head)
        terms[u, :, :, value_at] = dot(rounded, grad, tn).astype(BF16).reshape(n, rows, head)

    def r_arrive(u, s):
        d = ways(u % 2, s)
        arrive(inbox.at[u, pl.ds(d[0], len(d)), s], sent.at[1], r_recv.at[u, s])

    def r_step(u, s):
        if s > 0:
            r_arrive(u, s - 1)
        for d in ways(u % 2, s):
            owner = ring_index(place + sign[d] * (hops(n, d, u % 2) - s), n)
            src = terms.at[u, owner]
            if s > 0:
                src = inbox.at[u, d, s - 1]
                src[...] = (src[...].astype(F32) + terms[u, owner].astype(F32)).astype(BF16)
            send_on(src, inbox.at[u, d, s], sent.at[1], r_recv.at[u, s], d)

    def r_total(u):
        part, c = divmod(u, seqs)
        r_arrive(u, n // 2 - 1)
        result = terms[u, me].astype(F32)
        for d in (1 - u % 2, u % 2):
            result = result + inbox[u, d, hops(n, d, u % 2) - 1].astype(F32)
        at = slice(c * rows, (c + 1) * rows)
        for k in range(heads):
            back = result[:, k * head : (k + 1) * head]
            turned = pltpu.roll(back, head // 2, 1)
            back = (back * cos_ref[...] - turned * sin_ref[...]).astype(BF16)
            gall[u, dp, :, k * head : (k + 1) * head] = back
            own_kv[part, at, k * head : (k + 1) * head] = back
        back = result[:, width:].astype(BF16)
        gall[u, dp, :, width:] = back
        own_kv[part, at, width:] = back
        for o in range(1, m):
            slot = gall.at[u, dp]
            remote(slot, slot, sent.at[4], g_recv.at[part], "dp", (dp + o) % m).start()

    def product_step(part):
        slots = gall.at[pl.ds(part * seqs, seqs), pl.ds(0, m - 1)]
        remote(slots, slots, sent.at[4], g_recv.at[part], "dp", (dp + 1) % m).wait_recv()
        grads = gall[part * seqs : (part + 1) * seqs].reshape(seqs * m * rows, 2 * width)
        part2[part] = dot(xt[...], grads, nn).astype(BF16).reshape(n, own, 2 * width)

    def w_arrive(lane, half, s):
        d = ways(half, s)
        arrive(inbox2.at[lane, pl.ds(d[0], len(d)), s], sent.at[2], w_recv.at[lane, s])

    def w_step(part, half, s):
        lane = 2 * part + half
        if s > 0:
            w_arrive(lane, half, s - 1)
        for d in ways(half, s):
            owner = ring_index(place + sign[d] * (hops(n, d, half) - s), n)
            at = pl.ds(half * half_own, half_own)
            src = part2.at[part, owner, at]
            if s > 0:
                src = inbox2.at[lane, d, s - 1]
                src[...] = (src[...].astype(F32) + part2[part, owner, at].astype(F32)).astype(BF16)
            send_on(src, inbox2.at[lane, d, s], sent.at[2], w_recv.at[lane, s], d)

    def w_total(part, half):
        lane = 2 * part + half
        w_arrive(lane, half, n // 2 - 1)
        at = slice(half * half_own, (half + 1) * half_own)
        result = part2[part, me, at].astype(F32)
        for d in (1 - half, half):
            result = result + inbox2[lane, d, hops(n, d, half) - 1].astype(F32)
        gkw[at, part * width : (part + 1) * width] = result[:, :width]
        gvw[at, part * width : (part + 1) * width] = result[:, width:]

    state = {}

    def project_step(part, half):
        at = slice(half * model_width // 2, (half + 1) * model_width // 2)
        piece = dot(own_kv[part], wkv[part, at], nt)
        ng[:, at] = ng[:, at] + piece if part else piece

    def inner_step(q):
        at = slice(q * piece_width, (q + 1) * piece_width)
        wide = x_ref[:, :, at].reshape(count, piece_width).astype(F32)
        inner = jnp.sum(ng[:, at] * gain_ref[:, at] * wide, axis=1, keepdims=True)
        state["inner"] = state["inner"] + inner if q else inner

    def finish_step(q):
        at = slice(q * piece_width, (q + 1) * piece_width)
        rms = rms_ref[...].reshape(count, 1)
        slope = rms * rms * rms * (state["inner"] / model_width)
        wide = x_ref[:, :, at].reshape(count, piece_width).astype(F32)
        gx[:, at] = (rms * gain_ref[:, at] * ng[:, at] - wide * slope).astype(BF16)

    def gain_step():
        block = dp * n + me if permuted else me * m + dp
        at = pl.ds(pl.multiple_of(block * own, own), own)
        folded = jnp.zeros((own, width), F32)
        for part in range(PARTS):
            columns = slice(part * width, (part + 1) * width)
            folded = folded + wkv[part, at, :width].astype(F32) * gkw[:, columns]
            folded = folded + wkv[part, at, width:].astype(F32) * gvw[:, columns]
        gain_out[...] = jnp.sum(jnp.transpose(folded), axis=0, keepdims=True) / gain_rows[pl.ds(block, 1), :]

    def drain_step():
        rings = kv.at[:, pl.ds(0, n - 1)]
        lanes = part2.at[:, pl.ds(0, n - 1)]
        slices = xg.at[:, pl.ds(0, m - 1)]
        grads = gall.at[:, pl.ds(0, m - 1)]
        for i, ref in enumerate((rings, rings, lanes, slices, grads)):
            remote(ref, ref, sent.at[i], x_recv.at[0], "ctx", targets[0]).wait_send()

    steps = {
        "proj": proj_step,
        "A": a_step,
        "X": x_step,
        "mask": mask_step,
        "xwait": x_wait,
        "xt": transpose_step,
        "attend": attend_step,
        "R": r_step,
        "total": r_total,
        "drain": drain_step,
        "M": product_step,
        "W": w_step,
        "wtotal": w_total,
        "project": project_step,
        "inner": inner_step,
        "finish": finish_step,
        "gain": gain_step,
    }
    for kind, *where in plan(n, m, seqs, heads):
        steps[kind](*where)


def layer(n, m, permuted, span_order, norm_gain, tokens, key_weight, value_weight, queries, grads):
    seqs, rows, model_width = tokens.shape
    kv_width = key_weight.shape[1]
    own = model_width // (n * m)
    width = kv_width // PARTS
    units = PARTS * seqs
    count = seqs * rows
    starts, offsets = rotation_tables(2 * n, rows // 2)
    dma = pltpu.SemaphoreType.DMA
    out_shape = (
        jax.ShapeDtypeStruct(queries.shape, BF16),
        jax.ShapeDtypeStruct(queries.shape, BF16),
        jax.ShapeDtypeStruct((count, model_width), BF16),
        jax.ShapeDtypeStruct((own, kv_width), F32),
        jax.ShapeDtypeStruct((own, kv_width), F32),
        jax.ShapeDtypeStruct((1, own), F32),
    )
    vectors = [
        ((1, model_width), F32),
        ((n * m, own), F32),
        (tokens.shape, BF16),
        ((PARTS, model_width, 2 * width), BF16),
        (queries.shape, BF16),
        (queries.shape, BF16),
        ((m, seqs, rows, n * own), BF16),
        ((seqs, m, rows, n * own), BF16),
        ((n * own, seqs * m * rows), BF16),
        ((units, n, rows, 2 * width), BF16),
        ((units, n, rows, 2 * width), BF16),
        ((units, 2, n // 2, rows, 2 * width), BF16),
        ((units, m, rows, 2 * width), BF16),
        ((PARTS, count, 2 * width), BF16),
        ((PARTS, n, own, 2 * width), BF16),
        ((2 * PARTS, 2, n // 2, own // 2, 2 * width), BF16),
        ((seqs, rows, 1), F32),
        ((count, model_width), F32),
        ((rows, HEAD_DIM), F32),
        ((rows, HEAD_DIM), F32),
        ((rows, n * rows), F32),
    ]
    held = sum(int(np.prod(shape)) * jnp.dtype(kind).itemsize for shape, kind in vectors)
    limit = min(60 * MIB, held + 8 * MIB)
    ring = dma((units, n // 2))
    return pl.pallas_call(
        functools.partial(layer_kernel, n, m, permuted),
        out_shape=out_shape,
        in_specs=[HBM] * 10,
        out_specs=[VMEM] * 6,
        scratch_shapes=[
            pltpu.SMEM(span_order.shape, jnp.int32),
            pltpu.VMEM(starts.shape, F32),
            pltpu.VMEM(offsets.shape, F32),
            *[pltpu.VMEM(*spec) for spec in vectors],
            dma((5,)),
            dma((seqs,)),
            dma((PARTS,)),
            dma((2,)),
            dma((5,)),
            ring,
            ring,
            dma((2 * PARTS, n // 2)),
            dma((1,)),
            dma((PARTS,)),
        ],
        compiler_params=pltpu.CompilerParams(
            collective_id=0, has_side_effects=True, vmem_limit_bytes=limit
        ),
        name="layer",
    )(
        *[
            pltpu.with_memory_space_constraint(array, pltpu.HBM)
            for array in (
                span_order,
                jnp.asarray(starts),
                jnp.asarray(offsets),
                norm_gain[None, :],
                norm_gain.reshape(n * m, own),
                tokens,
                key_weight,
                value_weight,
                queries,
                grads,
            )
        ]
    )


def deliver_kernel(*refs):
    count = (len(refs) - 1) // 2
    sems = refs[-1]
    copies = [pltpu.make_async_copy(refs[i], refs[count + i], sems.at[i]) for i in range(count)]
    for copy in copies:
        copy.start()
    for copy in copies:
        copy.wait()


def deliver(*arrays):
    return pl.pallas_call(
        deliver_kernel,
        out_shape=tuple(jax.ShapeDtypeStruct(a.shape, a.dtype) for a in arrays),
        in_specs=[VMEM] * len(arrays),
        out_specs=[ANY] * len(arrays),
        scratch_shapes=[pltpu.SemaphoreType.DMA((len(arrays),))],
        compiler_params=pltpu.CompilerParams(vmem_limit_bytes=16 * MIB),
        name="deliver",
    )(*arrays)


def body(n, m, tokens, queries, d_attended, span_order, norm_gain, key_weight, value_weight):
    seqs, rows, model_width = tokens.shape
    own = model_width // (n * m)
    permuted = own % 128 != 0

    def shuffle(array, axis):
        shape = array.shape
        split = array.reshape(shape[:axis] + (n, m, own) + shape[axis + 1 :])
        return jnp.swapaxes(split, axis, axis + 1).reshape(shape)

    if permuted:
        tokens, norm_gain = shuffle(tokens, 2), shuffle(norm_gain, 0)
        key_weight, value_weight = shuffle(key_weight, 0), shuffle(value_weight, 0)
    attended, dquery, grad_rows, key_grad, value_grad, gain = deliver(
        *layer(n, m, permuted, span_order, norm_gain, tokens, key_weight, value_weight, queries, d_attended)
    )
    grad_rows = grad_rows.reshape(seqs, rows, model_width)
    if permuted:
        split = grad_rows.reshape(seqs, rows, m, n, own)
        grad_rows = jnp.swapaxes(split, 2, 3).reshape(seqs, rows, model_width)
    return attended, dquery, grad_rows, key_grad, value_grad, gain.reshape(own)


def solution(mesh):
    split = P("dp", "ctx", None)
    return jax.shard_map(
        functools.partial(body, mesh.shape["ctx"], mesh.shape["dp"]),
        mesh=mesh,
        in_specs=(split, split, split, P(), P(), P(), P()),
        out_specs=(
            split,
            split,
            split,
            P(("ctx", "dp"), None),
            P(("ctx", "dp"), None),
            P(("ctx", "dp")),
        ),
        check_vma=False,
    )
```

```python
import functools

import jax
import jax.numpy as jnp
import numpy as np
from jax import lax
from jax.experimental import pallas as pl
from jax.experimental.pallas import tpu as pltpu
from jax.sharding import PartitionSpec as P

HEAD_DIM = 128
ROPE_BASE = 500000.0
EPSILON = 1e-05
MESH = pl.DeviceIdType.MESH
VMEM = pl.BlockSpec(memory_space=pltpu.VMEM)
HBM = pl.BlockSpec(memory_space=pltpu.HBM)
ANY = pl.BlockSpec(memory_space=pl.ANY)
F32 = jnp.float32
BF16 = jnp.bfloat16
MIB = 1024 * 1024

PARTS = 4
PIECES = 4


def ring_place(index, n):
    return jnp.where(index % 2 == 0, index // 2, n - 1 - index // 2)


def ring_index(place, n):
    place = (place + 2 * n) % n
    return jnp.where(place < n // 2, 2 * place, 2 * (n - 1 - place) + 1)


def remote(src, dst, send, recv, axis, target):
    return pltpu.make_async_remote_copy(
        src_ref=src,
        dst_ref=dst,
        send_sem=send,
        recv_sem=recv,
        device_id={axis: target},
        device_id_type=MESH,
    )


def rotation_tables(spans, span_len):
    half = HEAD_DIM // 2
    frequency = ROPE_BASE ** (-2.0 * np.arange(half, dtype=np.float64) / HEAD_DIM)
    frequency = np.concatenate([frequency, frequency])

    def table(at):
        angle = at.astype(np.float64)[:, None] * frequency[None, :]
        return np.stack([np.cos(angle), np.sin(angle)]).astype(np.float32)

    return table(np.arange(spans) * span_len), table(np.arange(span_len))


class Task:
    def __init__(self, name, rank, cost, needs=(), waits=(), sends=()):
        self.name, self.rank, self.cost = name, rank, cost
        self.needs, self.waits, self.sends = needs, waits, sends


def arrange(tasks, latency):
    now, free, arrival, done, order = 0.0, {}, {}, set(), []
    left = list(tasks)
    while left:
        best = None
        for task in left:
            if all(name in done for name in task.needs) and all(key in arrival for key in task.waits):
                at = max([arrival[key] for key in task.waits], default=0.0)
                key = (max(at, now), task.rank)
                if best is None or key < best[0]:
                    best = (key, task)
        (at, _), task = best
        left.remove(task)
        now = at + task.cost
        done.add(task.name)
        order.append(task.name)
        for key, link, cost in task.sends:
            free[link] = max(free.get(link, 0.0), now) + cost
            arrival[key] = free[link] + latency
    return order


def hops(n, d, parity):
    return n // 2 if d == parity else n // 2 - 1


GATES = (None, 0, 2, 3)
LATENCY = 3.6
MESSAGE = 0.7
ATTEND = 1.02


def plan(n, m, seqs, heads):
    units = PARTS * seqs
    tasks = []

    def task(*args, **rest):
        tasks.append(Task(*args, **rest))

    def ways(parity, s):
        return [d for d in range(2) if s < hops(n, d, parity)]

    def ring(name, parity, rank, first):
        for s in range(n // 2):
            task(
                (*name, s),
                rank + s,
                0.03,
                needs=first if s == 0 else [],
                waits=[(*name, s - 1, d) for d in ways(parity, s - 1)] if s else [],
                sends=[((*name, s, d), d, MESSAGE) for d in ways(parity, s)],
            )

    def end(name, parity):
        return [(*name, n // 2 - 1, d) for d in ways(parity, n // 2 - 1)]

    for part in range(PARTS):
        task(("proj", part), 0.5, 0.75, needs=[("proj", part - 1)] if part else [])
        for c in range(seqs):
            u = part * seqs + c
            first = [("proj", part)] + ([("A", u - 1, 0)] if u else [])
            if GATES[part] is not None:
                first.append(("A", 0, GATES[part]))
            ring(("A", u), u % 2, 0.3 * part, first)
    task(
        ("X",),
        0.4,
        0.15,
        needs=[("A", seqs - 1, 0)],
        sends=[(("X", o), "x", 4 * PARTS * MESSAGE / 2) for o in range(1, m)],
    )
    task(("mask",), 40, 0.1, needs=[("proj", PARTS - 1)])
    task(
        ("xwait",),
        45,
        0.01,
        waits=[("X", o) for o in range(1, m)],
        needs=[("attend", 2 * seqs - 1, heads - 1)],
    )
    for c in range(seqs):
        task(("xt", c), 50 + c, 0.2, needs=[("xwait",)])
    for u in range(units):
        for k in range(heads):
            task(
                ("attend", u, k),
                20 + u + k / heads,
                ATTEND,
                needs=[("mask",)] if k == 0 else [("attend", u, k - 1)],
                waits=end(("A", u), u % 2) if k == 0 else [],
            )
        ring(("R", u), u % 2, 2 + 0.3 * (u // seqs), [("attend", u, heads - 1)])
        task(
            ("total", u),
            4 + u / units,
            0.1,
            waits=end(("R", u), u % 2),
            sends=[(("G", u, o), "x" if o > 1 else "chip", MESSAGE) for o in range(1, m)],
        )
    for part in range(PARTS):
        mine = [part * seqs + c for c in range(seqs)]
        task(
            ("M", part),
            11 + part,
            0.7,
            needs=[("xt", c) for c in range(seqs)],
            waits=[("G", u, o) for u in mine for o in range(1, m)],
        )
        for half in range(2):
            ring(("W", part, half), half, 2 + 0.3 * part, [("M", part)])
            task(("wtotal", part, half), 3, 0.05, waits=end(("W", part, half), half))
        for half in range(2):
            before = [("total", u) for u in mine] + ([("project", part - 1, half)] if part else [])
            task(("project", part, half), 60 + part + half / 2, 0.47, needs=before)
    projected = [("project", part, half) for part in range(PARTS) for half in range(2)]
    for q in range(PIECES):
        before = projected if q == 0 else [("inner", q - 1)]
        task(("inner", q), 70 + q, 0.13, needs=before)
        task(("finish", q), 80 + q, 0.17, needs=[("inner", PIECES - 1)])
    task(("gain",), 90, 0.13, needs=[("wtotal", part, half) for part in range(PARTS) for half in range(2)])
    task(("drain",), 99, 0.05, needs=[("gain",)] + [("finish", q) for q in range(PIECES)])
    return arrange(tasks, LATENCY)


def blocks_of(n, m, own, permuted):
    if permuted:
        return [(j * n * own, n * own, j, 0) for j in range(m)]
    return [(b * own, own, b % m, (b // m) * own) for b in range(n * m)]


def layer_kernel(
    n,
    m,
    permuted,
    span_hbm,
    start_hbm,
    offset_hbm,
    gain_hbm,
    rows_hbm,
    x_hbm,
    wk_hbm,
    wv_hbm,
    q_hbm,
    g_hbm,
    att,
    dq,
    gx,
    gkw,
    gvw,
    gain_out,
    span_ref,
    start_ref,
    offset_ref,
    gain_ref,
    gain_rows,
    x_ref,
    wkv,
    q_ref,
    g_ref,
    normed,
    xg,
    xt,
    kv,
    terms,
    inbox,
    gall,
    own_kv,
    part2,
    inbox2,
    rms_ref,
    ng,
    cos_ref,
    sin_ref,
    bias,
    ssem,
    xsem,
    wsem,
    qsem,
    sent,
    a_recv,
    r_recv,
    w_recv,
    x_recv,
    g_recv,
):
    me = lax.axis_index("ctx")
    dp = lax.axis_index("dp")
    place = ring_place(me, n)
    sign = (1, -1)
    targets = [ring_index(place + 1, n), ring_index(place - 1, n)]
    seqs, rows, _ = q_ref.shape
    kv_width = gkw.shape[1]
    model_width = x_ref.shape[2]
    count = seqs * rows
    own = gkw.shape[0]
    head = HEAD_DIM
    span_len = rows // 2
    width = kv_width // PARTS
    heads = width // head
    group = q_ref.shape[2] // kv_width
    scale = head ** (-0.5)
    units = PARTS * seqs
    half_own = own // 2
    nt = (((1,), (1,)), ((), ()))
    nn = (((1,), (0,)), ((), ()))
    tn = (((0,), (0,)), ((), ()))
    dot = functools.partial(lax.dot_general, preferred_element_type=F32)
    blocks = blocks_of(n, m, own, permuted)
    per_piece = len(blocks) // PIECES
    piece_width = model_width // PIECES

    def start(loads):
        for load in loads:
            load.start()
        return loads

    x_loads = start([pltpu.make_async_copy(x_hbm.at[c], x_ref.at[c], xsem.at[c]) for c in range(seqs)])
    small = (
        (gain_hbm, gain_ref),
        (span_hbm, span_ref),
        (start_hbm, start_ref),
        (offset_hbm, offset_ref),
        (rows_hbm, gain_rows),
    )
    small_loads = start([pltpu.make_async_copy(src, dst, ssem.at[i]) for i, (src, dst) in enumerate(small)])
    w_loads = [
        [
            pltpu.make_async_copy(
                src.at[:, pl.ds(part * width, width)], wkv.at[part, :, pl.ds(t * width, width)], wsem.at[part]
            )
            for t, src in enumerate((wk_hbm, wv_hbm))
        ]
        for part in range(PARTS)
    ]
    q_loads = [
        pltpu.make_async_copy(src, dst, qsem.at[t])
        for t, (src, dst) in enumerate(((q_hbm, q_ref), (g_hbm, g_ref)))
    ]
    start(w_loads[0])
    barrier = pltpu.get_barrier_semaphore()
    for axis, target in [("ctx", targets[0]), ("ctx", targets[1])] + [("dp", (dp + o) % m) for o in range(1, m)]:
        pl.semaphore_signal(barrier, inc=1, device_id={axis: target}, device_id_type=MESH)

    for c in range(seqs):
        x_loads[c].wait()
        if c == 0:
            for loads in w_loads[1:]:
                start(loads)
            start(q_loads)
            small_loads[0].wait()
        total = jnp.zeros((rows, 1), F32)
        for q in range(PIECES):
            wide = x_ref[c, :, q * piece_width : (q + 1) * piece_width].astype(F32)
            total = total + jnp.sum(wide * wide, axis=1, keepdims=True)
        rms = lax.rsqrt(total / model_width + EPSILON)
        rms_ref[c] = rms
        for start, size, j, offset in blocks:
            at = slice(start, start + size)
            value = (x_ref[c, :, at].astype(F32) * rms * gain_ref[:, at]).astype(BF16)
            normed[j, c, :, offset : offset + size] = value

    for load in small_loads[1:]:
        load.wait()
    offset_cos, offset_sin = offset_ref[0], offset_ref[1]
    lane = lax.broadcasted_iota(jnp.int32, (span_len, head), 1)
    signs = jnp.where(lane < head // 2, -1.0, 1.0).astype(F32)
    for half in range(2):
        span = span_ref[2 * me + half]
        start_cos = start_ref[0, pl.ds(span, 1), :]
        start_sin = start_ref[1, pl.ds(span, 1), :]
        at = slice(half * span_len, (half + 1) * span_len)
        cos_ref[at] = start_cos * offset_cos - start_sin * offset_sin
        sin_ref[at] = (start_sin * offset_cos + start_cos * offset_sin) * signs

    def proj_step(part):
        pltpu.make_async_copy(wkv.at[part], wkv.at[part], wsem.at[part]).wait()
        both = jnp.zeros((count, 2 * width), F32)
        for q in range(PIECES):
            lhs = jnp.concatenate(
                [
                    normed[j, :, :, offset : offset + size].reshape(count, size)
                    for _, size, j, offset in blocks[q * per_piece : (q + 1) * per_piece]
                ],
                axis=1,
            )
            both = both + dot(lhs, wkv[part, q * piece_width : (q + 1) * piece_width], nn)
        for c in range(seqs):
            u = part * seqs + c
            at = slice(c * rows, (c + 1) * rows)
            for k in range(heads):
                turn = both[at, k * head : (k + 1) * head]
                turned = pltpu.roll(turn, head // 2, 1)
                kv[u, me, :, k * head : (k + 1) * head] = (turn * cos_ref[...] + turned * sin_ref[...]).astype(BF16)
            kv[u, me, :, width : 2 * width] = both[at, width:].astype(BF16)
        if part == 0:
            pl.semaphore_wait(barrier, 2 + m - 1)

    def ways(parity, s):
        return [d for d in range(2) if s < hops(n, d, parity)]

    def arrive(ref, send, recv):
        remote(ref, ref, send, recv, "ctx", targets[0]).wait_recv()

    def send_on(src, dst, sends, recv, d):
        remote(src, dst, sends, recv, "ctx", targets[d]).start()

    def a_arrive(u, s):
        arrive(kv.at[u, pl.ds(0, len(ways(u % 2, s)))], sent.at[0], a_recv.at[u, s])

    def a_step(u, s):
        if s > 0:
            a_arrive(u, s - 1)
        for d in ways(u % 2, s):
            slot = kv.at[u, ring_index(place - sign[d] * s, n)]
            send_on(slot, slot, sent.at[0], a_recv.at[u, s], d)

    def x_step():
        for o in range(1, m):
            target = (dp + o) % m
            remote(normed.at[target], xg.at[:, dp], sent.at[3], x_recv.at[0], "dp", target).start()
        xg[:, dp] = normed[dp]

    def mask_step():
        for load in q_loads:
            load.wait()
        spans = 2 * n
        lane = lax.broadcasted_iota(jnp.int32, (1, n * rows), 1)
        key_pos = jnp.zeros((1, n * rows), jnp.int32)
        for k in range(spans):
            inside = (lane >= k * span_len) & (lane < (k + 1) * span_len)
            key_pos = jnp.where(inside, lane + (span_ref[k] - k) * span_len, key_pos)
        row = lax.broadcasted_iota(jnp.int32, (rows, 1), 0)
        first, second = span_ref[2 * me], span_ref[2 * me + 1]
        query_pos = row + jnp.where(row < span_len, first * span_len, (second - 1) * span_len)
        bias[...] = jnp.where(key_pos <= query_pos, 0.0, -1e30).astype(F32)

    def transpose_step(c):
        wide = xg[c].reshape(m * rows, n * own)
        xt[:, c * m * rows : (c + 1) * m * rows] = jnp.transpose(wide)

    def x_wait():
        slots = xg.at[:, pl.ds(0, m - 1)]
        remote(slots, slots, sent.at[3], x_recv.at[0], "dp", (dp + 1) % m).wait_recv()

    def attend_step(u, k):
        part, c = divmod(u, seqs)
        if k == 0:
            a_arrive(u, n // 2 - 1)
        first = ((part * heads + k) * group) * head
        columns = [slice(first + i * head, first + (i + 1) * head) for i in range(group)]
        query = jnp.concatenate([q_ref[c, :, column] for column in columns], axis=0)
        grad = jnp.concatenate([g_ref[c, :, column] for column in columns], axis=0)
        key_at = slice(k * head, (k + 1) * head)
        value_at = slice(width + k * head, width + (k + 1) * head)
        key = kv[u, :, :, key_at].reshape(n * rows, head)
        value = kv[u, :, :, value_at].reshape(n * rows, head)
        masked = jnp.concatenate([bias[...]] * group, axis=0)
        scores = dot(query, key, nt) * scale + masked
        exponent = jnp.exp(scores - jnp.max(scores, axis=1, keepdims=True))
        probability = exponent * (1.0 / jnp.sum(exponent, axis=1, keepdims=True))
        rounded = probability.astype(BF16)
        attended = dot(rounded, value, nn).astype(BF16)
        delta = jnp.sum(grad.astype(F32) * attended.astype(F32), axis=1, keepdims=True)
        dscores = (probability * (dot(grad, value, nt) - delta)).astype(BF16)
        dquery = (dot(dscores, key, nn) * scale).astype(BF16)
        for i in range(group):
            att[c, :, columns[i]] = attended[i * rows : (i + 1) * rows]
            dq[c, :, columns[i]] = dquery[i * rows : (i + 1) * rows]
        terms[u, :, :, key_at] = (dot(dscores, query, tn) * scale).astype(BF16).reshape(n, rows, head)
        terms[u, :, :, value_at] = dot(rounded, grad, tn).astype(BF16).reshape(n, rows, head)

    def r_arrive(u, s):
        d = ways(u % 2, s)
        arrive(inbox.at[u, pl.ds(d[0], len(d)), s], sent.at[1], r_recv.at[u, s])

    def r_step(u, s):
        if s > 0:
            r_arrive(u, s - 1)
        for d in ways(u % 2, s):
            owner = ring_index(place + sign[d] * (hops(n, d, u % 2) - s), n)
            src = terms.at[u, owner]
            if s > 0:
                src = inbox.at[u, d, s - 1]
                src[...] = (src[...].astype(F32) + terms[u, owner].astype(F32)).astype(BF16)
            send_on(src, inbox.at[u, d, s], sent.at[1], r_recv.at[u, s], d)

    def r_total(u):
        part, c = divmod(u, seqs)
        r_arrive(u, n // 2 - 1)
        result = terms[u, me].astype(F32)
        for d in (1 - u % 2, u % 2):
            result = result + inbox[u, d, hops(n, d, u % 2) - 1].astype(F32)
        at = slice(c * rows, (c + 1) * rows)
        for k in range(heads):
            back = result[:, k * head : (k + 1) * head]
            turned = pltpu.roll(back, head // 2, 1)
            back = (back * cos_ref[...] - turned * sin_ref[...]).astype(BF16)
            gall[u, dp, :, k * head : (k + 1) * head] = back
            own_kv[part, at, k * head : (k + 1) * head] = back
        back = result[:, width:].astype(BF16)
        gall[u, dp, :, width:] = back
        own_kv[part, at, width:] = back
        for o in range(1, m):
            slot = gall.at[u, dp]
            remote(slot, slot, sent.at[4], g_recv.at[part], "dp", (dp + o) % m).start()

    def product_step(part):
        slots = gall.at[pl.ds(part * seqs, seqs), pl.ds(0, m - 1)]
        remote(slots, slots, sent.at[4], g_recv.at[part], "dp", (dp + 1) % m).wait_recv()
        grads = gall[part * seqs : (part + 1) * seqs].reshape(seqs * m * rows, 2 * width)
        part2[part] = dot(xt[...], grads, nn).astype(BF16).reshape(n, own, 2 * width)

    def w_arrive(lane, half, s):
        d = ways(half, s)
        arrive(inbox2.at[lane, pl.ds(d[0], len(d)), s], sent.at[2], w_recv.at[lane, s])

    def w_step(part, half, s):
        lane = 2 * part + half
        if s > 0:
            w_arrive(lane, half, s - 1)
        for d in ways(half, s):
            owner = ring_index(place + sign[d] * (hops(n, d, half) - s), n)
            at = pl.ds(half * half_own, half_own)
            src = part2.at[part, owner, at]
            if s > 0:
                src = inbox2.at[lane, d, s - 1]
                src[...] = (src[...].astype(F32) + part2[part, owner, at].astype(F32)).astype(BF16)
            send_on(src, inbox2.at[lane, d, s], sent.at[2], w_recv.at[lane, s], d)

    def w_total(part, half):
        lane = 2 * part + half
        w_arrive(lane, half, n // 2 - 1)
        at = slice(half * half_own, (half + 1) * half_own)
        result = part2[part, me, at].astype(F32)
        for d in (1 - half, half):
            result = result + inbox2[lane, d, hops(n, d, half) - 1].astype(F32)
        gkw[at, part * width : (part + 1) * width] = result[:, :width]
        gvw[at, part * width : (part + 1) * width] = result[:, width:]

    state = {}

    def project_step(part, half):
        at = slice(half * model_width // 2, (half + 1) * model_width // 2)
        piece = dot(own_kv[part], wkv[part, at], nt)
        ng[:, at] = ng[:, at] + piece if part else piece

    def inner_step(q):
        at = slice(q * piece_width, (q + 1) * piece_width)
        wide = x_ref[:, :, at].reshape(count, piece_width).astype(F32)
        inner = jnp.sum(ng[:, at] * gain_ref[:, at] * wide, axis=1, keepdims=True)
        state["inner"] = state["inner"] + inner if q else inner

    def finish_step(q):
        at = slice(q * piece_width, (q + 1) * piece_width)
        rms = rms_ref[...].reshape(count, 1)
        slope = rms * rms * rms * (state["inner"] / model_width)
        wide = x_ref[:, :, at].reshape(count, piece_width).astype(F32)
        gx[:, at] = (rms * gain_ref[:, at] * ng[:, at] - wide * slope).astype(BF16)

    def gain_step():
        block = dp * n + me if permuted else me * m + dp
        at = pl.ds(pl.multiple_of(block * own, own), own)
        folded = jnp.zeros((own, width), F32)
        for part in range(PARTS):
            columns = slice(part * width, (part + 1) * width)
            folded = folded + wkv[part, at, :width].astype(F32) * gkw[:, columns]
            folded = folded + wkv[part, at, width:].astype(F32) * gvw[:, columns]
        gain_out[...] = jnp.sum(jnp.transpose(folded), axis=0, keepdims=True) / gain_rows[pl.ds(block, 1), :]

    def drain_step():
        rings = kv.at[:, pl.ds(0, n - 1)]
        lanes = part2.at[:, pl.ds(0, n - 1)]
        slices = xg.at[:, pl.ds(0, m - 1)]
        grads = gall.at[:, pl.ds(0, m - 1)]
        for i, ref in enumerate((rings, rings, lanes, slices, grads)):
            remote(ref, ref, sent.at[i], x_recv.at[0], "ctx", targets[0]).wait_send()

    steps = {
        "proj": proj_step,
        "A": a_step,
        "X": x_step,
        "mask": mask_step,
        "xwait": x_wait,
        "xt": transpose_step,
        "attend": attend_step,
        "R": r_step,
        "total": r_total,
        "drain": drain_step,
        "M": product_step,
        "W": w_step,
        "wtotal": w_total,
        "project": project_step,
        "inner": inner_step,
        "finish": finish_step,
        "gain": gain_step,
    }
    for kind, *where in plan(n, m, seqs, heads):
        steps[kind](*where)


def layer(n, m, permuted, span_order, norm_gain, tokens, key_weight, value_weight, queries, grads):
    seqs, rows, model_width = tokens.shape
    kv_width = key_weight.shape[1]
    own = model_width // (n * m)
    width = kv_width // PARTS
    units = PARTS * seqs
    count = seqs * rows
    starts, offsets = rotation_tables(2 * n, rows // 2)
    dma = pltpu.SemaphoreType.DMA
    out_shape = (
        jax.ShapeDtypeStruct(queries.shape, BF16),
        jax.ShapeDtypeStruct(queries.shape, BF16),
        jax.ShapeDtypeStruct((count, model_width), BF16),
        jax.ShapeDtypeStruct((own, kv_width), F32),
        jax.ShapeDtypeStruct((own, kv_width), F32),
        jax.ShapeDtypeStruct((1, own), F32),
    )
    vectors = [
        ((1, model_width), F32),
        ((n * m, own), F32),
        (tokens.shape, BF16),
        ((PARTS, model_width, 2 * width), BF16),
        (queries.shape, BF16),
        (queries.shape, BF16),
        ((m, seqs, rows, n * own), BF16),
        ((seqs, m, rows, n * own), BF16),
        ((n * own, seqs * m * rows), BF16),
        ((units, n, rows, 2 * width), BF16),
        ((units, n, rows, 2 * width), BF16),
        ((units, 2, n // 2, rows, 2 * width), BF16),
        ((units, m, rows, 2 * width), BF16),
        ((PARTS, count, 2 * width), BF16),
        ((PARTS, n, own, 2 * width), BF16),
        ((2 * PARTS, 2, n // 2, own // 2, 2 * width), BF16),
        ((seqs, rows, 1), F32),
        ((count, model_width), F32),
        ((rows, HEAD_DIM), F32),
        ((rows, HEAD_DIM), F32),
        ((rows, n * rows), F32),
    ]
    held = sum(int(np.prod(shape)) * jnp.dtype(kind).itemsize for shape, kind in vectors)
    limit = min(60 * MIB, held + 8 * MIB)
    ring = dma((units, n // 2))
    return pl.pallas_call(
        functools.partial(layer_kernel, n, m, permuted),
        out_shape=out_shape,
        in_specs=[HBM] * 10,
        out_specs=[VMEM] * 6,
        scratch_shapes=[
            pltpu.SMEM(span_order.shape, jnp.int32),
            pltpu.VMEM(starts.shape, F32),
            pltpu.VMEM(offsets.shape, F32),
            *[pltpu.VMEM(*spec) for spec in vectors],
            dma((5,)),
            dma((seqs,)),
            dma((PARTS,)),
            dma((2,)),
            dma((5,)),
            ring,
            ring,
            dma((2 * PARTS, n // 2)),
            dma((1,)),
            dma((PARTS,)),
        ],
        compiler_params=pltpu.CompilerParams(
            collective_id=0, has_side_effects=True, vmem_limit_bytes=limit
        ),
        name="layer",
    )(
        *[
            pltpu.with_memory_space_constraint(array, pltpu.HBM)
            for array in (
                span_order,
                jnp.asarray(starts),
                jnp.asarray(offsets),
                norm_gain[None, :],
                norm_gain.reshape(n * m, own),
                tokens,
                key_weight,
                value_weight,
                queries,
                grads,
            )
        ]
    )


def deliver_kernel(*refs):
    count = (len(refs) - 1) // 2
    sems = refs[-1]
    copies = [pltpu.make_async_copy(refs[i], refs[count + i], sems.at[i]) for i in range(count)]
    for copy in copies:
        copy.start()
    for copy in copies:
        copy.wait()


def deliver(*arrays):
    return pl.pallas_call(
        deliver_kernel,
        out_shape=tuple(jax.ShapeDtypeStruct(a.shape, a.dtype) for a in arrays),
        in_specs=[VMEM] * len(arrays),
        out_specs=[ANY] * len(arrays),
        scratch_shapes=[pltpu.SemaphoreType.DMA((len(arrays),))],
        compiler_params=pltpu.CompilerParams(vmem_limit_bytes=16 * MIB),
        name="deliver",
    )(*arrays)


def body(n, m, tokens, queries, d_attended, span_order, norm_gain, key_weight, value_weight):
    seqs, rows, model_width = tokens.shape
    own = model_width // (n * m)
    permuted = own % 128 != 0

    def shuffle(array, axis):
        shape = array.shape
        split = array.reshape(shape[:axis] + (n, m, own) + shape[axis + 1 :])
        return jnp.swapaxes(split, axis, axis + 1).reshape(shape)

    if permuted:
        tokens, norm_gain = shuffle(tokens, 2), shuffle(norm_gain, 0)
        key_weight, value_weight = shuffle(key_weight, 0), shuffle(value_weight, 0)
    attended, dquery, grad_rows, key_grad, value_grad, gain = deliver(
        *layer(n, m, permuted, span_order, norm_gain, tokens, key_weight, value_weight, queries, d_attended)
    )
    grad_rows = grad_rows.reshape(seqs, rows, model_width)
    if permuted:
        split = grad_rows.reshape(seqs, rows, m, n, own)
        grad_rows = jnp.swapaxes(split, 2, 3).reshape(seqs, rows, model_width)
    return attended, dquery, grad_rows, key_grad, value_grad, gain.reshape(own)


def solution(mesh):
    split = P("dp", "ctx", None)
    return jax.shard_map(
        functools.partial(body, mesh.shape["ctx"], mesh.shape["dp"]),
        mesh=mesh,
        in_specs=(split, split, split, P(), P(), P(), P()),
        out_specs=(
            split,
            split,
            split,
            P(("ctx", "dp"), None),
            P(("ctx", "dp"), None),
            P(("ctx", "dp")),
        ),
        check_vma=False,
    )
```
